8 devices in a mesh: rep: 1 (over z), tp: 2 (over y), sp: 4 (over x, core).
Axes of the slice: x: 2, y: 2, z: 1, core: 2. Of those that a mesh axis runs over, the one named last changes fastest.
Arguments:
- x_in: bfloat16 [4096, 3072], P(('rep', 'sp'))
- positions: int32 [4096], P(('rep', 'sp'))
- segments: int32 [4096], P(('rep', 'sp'))
- gain_attn: float32 [3072], replicated
- w_q: bfloat16 [3072, 3072], P(None, 'tp')
- w_k: bfloat16 [3072, 1024], P(None, 'tp')
- w_v: bfloat16 [3072, 1024], P(None, 'tp')
- w_o: bfloat16 [3072, 3072], P('tp')
- gain_mlp: float32 [3072], replicated
- w_gate: bfloat16 [3072, 8192], P(None, 'tp')
- w_up: bfloat16 [3072, 8192], P(None, 'tp')
- w_down: bfloat16 [8192, 3072], P('tp')
Outputs:
- output 1: bfloat16 [4096, 3072], P(('rep', 'sp'))
- output 2: bfloat16 [4096, 8, 128], P('rep', ('tp', 'sp'))
- output 3: bfloat16 [4096, 8, 128], P('rep', ('tp', 'sp'))
All inputs are finite; a program needn't handle non-finite values.
Results may differ from the reference program's by a relative error of at most 0.00699993.
Values are sent between devices in bfloat16 or wider.
A program may use at most 1 GiB of HBM per device.

```python
import jax
import jax.numpy as jnp
from jax import lax

TOKENS = 4096
MODEL_DIM = 3072
FF_DIM = 8192
Q_HEADS = 24
KV_HEADS = 8
HEAD_DIM = 128
NUM_REQS = 2
KV_SLOTS = 8
ROPE_BASE = 500000
NORM_EPS = 1e-5


def draw_layout(layout_key):
    cut_key, step_key, start_key = jax.random.split(layout_key, 3)
    cut_rows = jnp.sort(jax.random.choice(cut_key, TOKENS - 1, (NUM_REQS - 1,), replace=False) + 1).astype(jnp.int32)
    tok_index = jnp.arange(TOKENS, dtype=jnp.int32)
    segments = jnp.sum(tok_index[:, None] >= cut_rows[None, :], axis=1).astype(jnp.int32)
    step_sizes = jax.random.randint(step_key, (TOKENS,), 1, 4, dtype=jnp.int32)
    run_sum = jnp.cumsum(step_sizes)
    first_rows = jnp.concatenate([jnp.zeros((1,), jnp.int32), cut_rows])
    seg_base = run_sum[first_rows] - step_sizes[first_rows]
    start_pos = jax.random.randint(start_key, (NUM_REQS,), 0, 1024, dtype=jnp.int32)
    positions = (run_sum - seg_base[segments] + start_pos[segments]).astype(jnp.int32)
    return positions, segments


def setup_inputs(seed: int = 0, part: int = 0) -> dict:
    base_key = jax.random.key(seed)
    part_key = jax.random.fold_in(base_key, part)
    x_key, layout_key = jax.random.split(part_key, 2)
    w_keys = jax.random.split(base_key, 10)
    positions, segments = draw_layout(layout_key)
    d_scale = MODEL_DIM ** -0.5

    def normal_weight(key_w, shape, std_dev):
        return (jax.random.normal(key_w, shape, jnp.float32) * std_dev).astype(jnp.bfloat16)

    return {
        "x_in": jax.random.normal(x_key, (TOKENS, MODEL_DIM), jnp.float32).astype(jnp.bfloat16),
        "positions": positions,
        "segments": segments,
        "gain_attn": 1.0 + 0.25 * jax.random.normal(w_keys[0], (MODEL_DIM,), jnp.float32),
        "w_q": normal_weight(w_keys[1], (MODEL_DIM, Q_HEADS * HEAD_DIM), 1.6 * d_scale),
        "w_k": normal_weight(w_keys[2], (MODEL_DIM, KV_HEADS * HEAD_DIM), 1.6 * d_scale),
        "w_v": normal_weight(w_keys[3], (MODEL_DIM, KV_HEADS * HEAD_DIM), d_scale),
        "w_o": normal_weight(w_keys[4], (Q_HEADS * HEAD_DIM, MODEL_DIM), (Q_HEADS * HEAD_DIM) ** -0.5),
        "gain_mlp": 1.0 + 0.25 * jax.random.normal(w_keys[5], (MODEL_DIM,), jnp.float32),
        "w_gate": normal_weight(w_keys[6], (MODEL_DIM, FF_DIM), d_scale),
        "w_up": normal_weight(w_keys[7], (MODEL_DIM, FF_DIM), d_scale),
        "w_down": normal_weight(w_keys[8], (FF_DIM, MODEL_DIM), FF_DIM ** -0.5),
    }


def rms_norm(x_f32, gain_vec):
    mean_sq = jnp.mean(x_f32 * x_f32, axis=-1, keepdims=True)
    return (x_f32 * lax.rsqrt(mean_sq + NORM_EPS) * gain_vec).astype(jnp.bfloat16)


def rope_tables(positions):
    half_dim = HEAD_DIM // 2
    inv_freq = jnp.power(jnp.float32(ROPE_BASE), -jnp.arange(half_dim, dtype=jnp.float32) * (2.0 / HEAD_DIM))
    angles = positions.astype(jnp.float32)[:, None] * inv_freq[None, :]
    return jnp.cos(angles)[:, None, :], jnp.sin(angles)[:, None, :]


def rotate(t_f32, cos_t, sin_t):
    half_dim = HEAD_DIM // 2
    t_lo = t_f32[..., :half_dim]
    t_hi = t_f32[..., half_dim:]
    return jnp.concatenate([t_lo * cos_t - t_hi * sin_t, t_hi * cos_t + t_lo * sin_t], axis=-1)


def reference(x_in, positions, segments, gain_attn, w_q, w_k, w_v, w_o, gain_mlp, w_gate, w_up, w_down):
    x_f32 = x_in.astype(jnp.float32)
    u_norm = rms_norm(x_f32, gain_attn)
    cos_t, sin_t = rope_tables(positions)
    q_rot = rotate(jnp.dot(u_norm, w_q, preferred_element_type=jnp.float32).reshape(TOKENS, Q_HEADS, HEAD_DIM), cos_t, sin_t).astype(jnp.bfloat16)
    k_rot = rotate(jnp.dot(u_norm, w_k, preferred_element_type=jnp.float32).reshape(TOKENS, KV_HEADS, HEAD_DIM), cos_t, sin_t).astype(jnp.bfloat16)
    v_proj = jnp.dot(u_norm, w_v, preferred_element_type=jnp.float32).astype(jnp.bfloat16).reshape(TOKENS, KV_HEADS, HEAD_DIM)
    group_size = Q_HEADS // KV_HEADS
    tok_index = jnp.arange(TOKENS)
    allowed = (tok_index[:, None] >= tok_index[None, :]) & (segments[:, None] == segments[None, :])
    score_scale = HEAD_DIM ** -0.5

    def one_head(operands):
        q_one, k_one, v_one = operands
        scores = jnp.dot(q_one, k_one.T, preferred_element_type=jnp.float32) * score_scale
        scores = jnp.where(allowed, scores, -1e30)
        prob_bf16 = jax.nn.softmax(scores, axis=-1).astype(jnp.bfloat16)
        return jnp.dot(prob_bf16, v_one, preferred_element_type=jnp.float32).astype(jnp.bfloat16)

    q_heads = jnp.transpose(q_rot, (1, 0, 2))
    k_heads = jnp.repeat(jnp.transpose(k_rot, (1, 0, 2)), group_size, axis=0)
    v_heads = jnp.repeat(jnp.transpose(v_proj, (1, 0, 2)), group_size, axis=0)
    attn_out = jnp.transpose(lax.map(one_head, (q_heads, k_heads, v_heads)), (1, 0, 2)).reshape(TOKENS, Q_HEADS * HEAD_DIM)
    x_mid = x_f32 + jnp.dot(attn_out, w_o, preferred_element_type=jnp.float32)
    u_mlp = rms_norm(x_mid, gain_mlp)
    gate_act = jnp.dot(u_mlp, w_gate, preferred_element_type=jnp.float32)
    up_act = jnp.dot(u_mlp, w_up, preferred_element_type=jnp.float32)
    hidden = (jax.nn.silu(gate_act) * up_act).astype(jnp.bfloat16)
    y_out = (x_mid + jnp.dot(hidden, w_down, preferred_element_type=jnp.float32)).astype(jnp.bfloat16)
    slot_repeat = KV_SLOTS // KV_HEADS
    return y_out, jnp.repeat(k_rot, slot_repeat, axis=1), jnp.repeat(v_proj, slot_repeat, axis=1)
```

```python
import functools
import jax
import jax.numpy as jnp
from jax import lax
from jax.experimental import pallas as pl
from jax.experimental.pallas import tpu as pltpu
from jax.sharding import PartitionSpec as P

HEAD_DIM = 128
HALF = HEAD_DIM // 2
ROPE_BASE = 500000.0
NORM_EPS = 1e-5
LOG2E = 1.4426950408889634
BF16 = jnp.bfloat16
F32 = jnp.float32

CHUNKS = 2
Q_BLOCK = 256
K_BLOCK = 512
FF_BLOCK = 512
MASKED = -1e30


def params(semantics, mib):
    return pltpu.CompilerParams(dimension_semantics=semantics, vmem_limit_bytes=mib << 20)


def dot(a, b):
    return jnp.dot(a, b, preferred_element_type=F32)


def normed(x, gain):
    mean_sq = jnp.mean(x * x, axis=-1, keepdims=True)
    return (x * lax.rsqrt(mean_sq + NORM_EPS) * gain).astype(BF16)


def rope_tables(positions):
    inv_freq = jnp.power(jnp.float32(ROPE_BASE), -jnp.arange(HALF, dtype=F32) * (2.0 / HEAD_DIM))
    angles = positions.astype(F32)[:, None] * inv_freq
    cos_t, sin_t = jnp.cos(angles), jnp.sin(angles)
    return jnp.concatenate([cos_t, cos_t], axis=-1), jnp.concatenate([-sin_t, sin_t], axis=-1)


def store_rotated(out_ref, rows, t_f32, cos_t, sin_t):
    for head in range(t_f32.shape[1] // HEAD_DIM):
        cols = slice(head * HEAD_DIM, (head + 1) * HEAD_DIM)
        t_head = t_f32[:, cols]
        out_ref[rows, cols] = (t_head * cos_t + pltpu.roll(t_head, HALF, 1) * sin_t).astype(BF16)


def kv_kernel(x_ref, gain_ref, wk_ref, wv_ref, cos_ref, sin_ref, u_ref, kv_ref):
    u = normed(x_ref[...].astype(F32), gain_ref[...])
    u_ref[...] = u
    width = wk_ref.shape[1]
    store_rotated(kv_ref, slice(None), dot(u, wk_ref[...]), cos_ref[...], sin_ref[...])
    kv_ref[:, width:] = dot(u, wv_ref[...]).astype(BF16)


def project_kv(x, gain, w_k, w_v, cos_t, sin_t):
    rows, dim = x.shape
    width = w_k.shape[1]
    block = 256
    whole = lambda a, b: pl.BlockSpec((a, b), lambda i: (0, 0))
    banded = lambda b: pl.BlockSpec((block, b), lambda i: (i, 0))
    return pl.pallas_call(
        kv_kernel, grid=(rows // block,), name="project_kv",
        in_specs=[banded(dim), whole(1, dim), whole(dim, width), whole(dim, width), banded(HEAD_DIM), banded(HEAD_DIM)],
        out_specs=[banded(dim), banded(2 * width)],
        out_shape=[jax.ShapeDtypeStruct((rows, dim), BF16), jax.ShapeDtypeStruct((rows, 2 * width), BF16)],
        compiler_params=params(("arbitrary",), 48),
        cost_estimate=pl.CostEstimate(flops=4 * rows * dim * width, bytes_accessed=4 * dim * (rows + width), transcendentals=0),
    )(x, gain, w_k, w_v, cos_t, sin_t)


def q_kernel(u_ref, w_ref, cos_ref, sin_ref, q_ref):
    block = 256

    @pl.loop(0, u_ref.shape[0] // block)
    def _(i):
        rows = pl.ds(pl.multiple_of(i * block, block), block)
        store_rotated(q_ref, rows, dot(u_ref[rows, :], w_ref[...]), cos_ref[rows, :], sin_ref[rows, :])


def project_q(u, w_q, cos_t, sin_t):
    rows, dim = u.shape
    width = w_q.shape[1]
    block = 512
    return pl.pallas_call(
        q_kernel, grid=(width // block,), name="project_q",
        in_specs=[pl.BlockSpec((rows, dim), lambda i: (0, 0)), pl.BlockSpec((dim, block), lambda i: (0, i)),
                  pl.BlockSpec((rows, HEAD_DIM), lambda i: (0, 0)), pl.BlockSpec((rows, HEAD_DIM), lambda i: (0, 0))],
        out_specs=pl.BlockSpec((rows, block), lambda i: (0, i)),
        out_shape=jax.ShapeDtypeStruct((rows, width), BF16),
        compiler_params=params(("arbitrary",), 48),
        cost_estimate=pl.CostEstimate(flops=2 * rows * dim * width, bytes_accessed=2 * dim * (rows + width), transcendentals=0),
    )(u, w_q, cos_t, sin_t)


def attn_kernel(group, row_base, meta_ref, q_ref, *refs):
    parts = (len(refs) - 6) // 2
    k_refs, v_refs = refs[:parts], refs[parts:2 * parts]
    o_ref, k_all, v_all, m_ref, l_ref, acc_ref = refs[2 * parts:]
    shard, cut = meta_ref[0], meta_ref[1]
    block = q_ref.shape[0]
    keys = k_refs[0].shape[0]
    scale = (HEAD_DIM ** -0.5) * LOG2E

    @pl.when(pl.program_id(1) == 0)
    def _():
        for idx in range(parts):
            rows = pl.ds(pl.multiple_of((shard ^ idx) * keys, keys), keys)
            k_all[rows, :] = k_refs[idx][...]
            v_all[rows, :] = v_refs[idx][...]

    first = shard * keys + row_base + pl.program_id(1) * block
    last = first + block - 1
    m_ref[...] = jnp.full_like(m_ref, MASKED)
    l_ref[...] = jnp.zeros_like(l_ref)
    acc_ref[...] = jnp.zeros_like(acc_ref)

    def step(masked, kb, carry):
        start = pl.multiple_of(kb * K_BLOCK, K_BLOCK)
        k_blk = k_all[pl.ds(start, K_BLOCK), :]
        v_blk = v_all[pl.ds(start, K_BLOCK), :]
        if masked:
            r_idx = first + lax.broadcasted_iota(jnp.int32, (block, K_BLOCK), 0)
            k_idx = start + lax.broadcasted_iota(jnp.int32, (block, K_BLOCK), 1)
            allowed = (k_idx <= r_idx) & ((k_idx >= cut) | (r_idx < cut))
        for head in range(group):
            s = lax.dot_general(q_ref[:, head * HEAD_DIM:(head + 1) * HEAD_DIM], k_blk,
                                (((1,), (1,)), ((), ())), preferred_element_type=F32) * scale
            if masked:
                s = jnp.where(allowed, s, MASKED)
            m_old = m_ref[head]
            m_new = jnp.maximum(m_old, jnp.max(s, axis=1, keepdims=True))
            alpha = jnp.exp2(m_old - m_new)
            p = jnp.exp2(s - jnp.concatenate([m_new] * (K_BLOCK // HEAD_DIM), axis=1))
            l_part = p[:, :HEAD_DIM]
            for lane in range(1, K_BLOCK // HEAD_DIM):
                l_part = l_part + p[:, lane * HEAD_DIM:(lane + 1) * HEAD_DIM]
            m_ref[head] = m_new
            l_ref[head] = alpha * l_ref[head] + l_part
            acc_ref[head] = alpha * acc_ref[head] + dot(p.astype(BF16), v_blk)
        return carry

    low = jnp.where(first >= cut, cut, 0) // K_BLOCK
    high = last // K_BLOCK + 1
    clear = (jnp.where(last >= cut, cut, 0) + K_BLOCK - 1) // K_BLOCK
    edge_a = jnp.minimum(jnp.maximum(clear, low), high)
    edge_b = jnp.maximum(edge_a, (first + 1) // K_BLOCK)
    lax.fori_loop(low, edge_a, functools.partial(step, True), 0)
    lax.fori_loop(edge_a, edge_b, functools.partial(step, False), 0)
    lax.fori_loop(edge_b, high, functools.partial(step, True), 0)
    for head in range(group):
        total = jnp.sum(l_ref[head], axis=1, keepdims=True)
        o_ref[:, head * HEAD_DIM:(head + 1) * HEAD_DIM] = (acc_ref[head] / total).astype(BF16)


def attention(meta, q_rot, kv_parts, row_base, rows, flops):
    kv_rows, kv_width = kv_parts[0].shape
    kv_heads = kv_width // (2 * HEAD_DIM)
    group = q_rot.shape[1] // HEAD_DIM // kv_heads
    width = group * HEAD_DIM
    parts = len(kv_parts)
    base = row_base // Q_BLOCK
    k_spec = pl.BlockSpec((kv_rows, HEAD_DIM), lambda h, i, m: (0, h))
    v_spec = pl.BlockSpec((kv_rows, HEAD_DIM), lambda h, i, m: (0, kv_heads + h))
    return pl.pallas_call(
        functools.partial(attn_kernel, group, row_base), name="attention",
        grid_spec=pltpu.PrefetchScalarGridSpec(
            num_scalar_prefetch=1, grid=(kv_heads, rows // Q_BLOCK),
            in_specs=[pl.BlockSpec((Q_BLOCK, width), lambda h, i, m: (base + i, h))] + [k_spec] * parts + [v_spec] * parts,
            out_specs=pl.BlockSpec((Q_BLOCK, width), lambda h, i, m: (i, h)),
            scratch_shapes=[pltpu.VMEM((parts * kv_rows, HEAD_DIM), BF16), pltpu.VMEM((parts * kv_rows, HEAD_DIM), BF16)]
                           + [pltpu.VMEM((group, Q_BLOCK, HEAD_DIM), F32)] * 3),
        out_shape=jax.ShapeDtypeStruct((rows, kv_heads * width), BF16),
        compiler_params=params(("arbitrary", "arbitrary"), 48),
        cost_estimate=pl.CostEstimate(flops=flops, bytes_accessed=16 << 20, transcendentals=0),
    )(meta, q_rot, *kv_parts, *kv_parts)


def mid_kernel(meta_ref, x_ref, a_ref, b_ref, wa_ref, wb_ref, gain_ref, u_ref, own_ref, mid_ref):
    step = pl.program_id(0)
    width = wa_ref.shape[1]
    cols = pl.ds(pl.multiple_of(step * width, width), width)
    mid_ref[:, cols] = x_ref[...].astype(F32) + (dot(a_ref[...], wa_ref[...]) + dot(b_ref[...], wb_ref[...]))

    @pl.when(step == pl.num_programs(0) - 1)
    def _():
        half = own_ref.shape[0]
        own_ref[...] = mid_ref[pl.ds(pl.multiple_of(meta_ref[2] * half, half), half), :]
        block = 128

        @pl.loop(0, u_ref.shape[0] // block)
        def _(i):
            rows = pl.ds(pl.multiple_of(i * block, block), block)
            u_ref[rows, :] = normed(mid_ref[rows, :], gain_ref[...])


def attn_out(meta, x, chunk, attn_mine, attn_peer, wo_mine, wo_peer, gain):
    rows, depth = attn_mine.shape
    dim = x.shape[1]
    block = 512
    resident = lambda a, b: pl.BlockSpec((a, b), lambda i, m: (0, 0))
    return pl.pallas_call(
        mid_kernel, name="attn_out",
        grid_spec=pltpu.PrefetchScalarGridSpec(
            num_scalar_prefetch=1, grid=(dim // block,),
            in_specs=[pl.BlockSpec((rows, block), lambda i, m: (chunk, i)), resident(rows, depth), resident(rows, depth),
                      pl.BlockSpec((depth, block), lambda i, m: (0, i)), pl.BlockSpec((depth, block), lambda i, m: (0, i)),
                      resident(1, dim)],
            out_specs=[resident(rows, dim), resident(rows // 2, dim)],
            scratch_shapes=[pltpu.VMEM((rows, dim), F32)]),
        out_shape=[jax.ShapeDtypeStruct((rows, dim), BF16), jax.ShapeDtypeStruct((rows // 2, dim), F32)],
        compiler_params=params(("arbitrary",), 56),
        cost_estimate=pl.CostEstimate(flops=4 * rows * depth * dim, bytes_accessed=4 * depth * dim, transcendentals=0),
    )(meta, x, attn_mine, attn_peer, wo_mine, wo_peer, gain)


def mlp_kernel(meta_ref, u_ref, wg_ref, wu_ref, wd_ref, p_ref):
    u = u_ref[...]
    gate = dot(u, wg_ref[...])
    hidden = (gate * jax.nn.sigmoid(gate) * dot(u, wu_ref[...])).astype(BF16)

    @pl.when(pl.program_id(0) == 0)
    def _():
        p_ref[...] = dot(hidden, wd_ref[...])

    @pl.when(pl.program_id(0) > 0)
    def _():
        p_ref[...] += dot(hidden, wd_ref[...])


def mlp_part(meta, slot, u_chunk, w_gate, w_up, w_down):
    dim, ff = w_gate.shape
    rows = u_chunk.shape[0] // 2
    return pl.pallas_call(
        mlp_kernel, name="mlp_part",
        grid_spec=pltpu.PrefetchScalarGridSpec(
            num_scalar_prefetch=1, grid=(ff // FF_BLOCK,),
            in_specs=[pl.BlockSpec((rows, dim), lambda i, m: (m[slot], 0)),
                      pl.BlockSpec((dim, FF_BLOCK), lambda i, m: (0, i)), pl.BlockSpec((dim, FF_BLOCK), lambda i, m: (0, i)),
                      pl.BlockSpec((FF_BLOCK, dim), lambda i, m: (i, 0))],
            out_specs=pl.BlockSpec((rows, dim), lambda i, m: (0, 0))),
        out_shape=jax.ShapeDtypeStruct((rows, dim), F32),
        compiler_params=params(("arbitrary",), 56),
        cost_estimate=pl.CostEstimate(flops=6 * rows * dim * ff, bytes_accessed=6 * dim * ff, transcendentals=0),
    )(meta, u_chunk, w_gate, w_up, w_down)


def solution(mesh):
    sp_size = mesh.shape["sp"]
    row_spec = P(("rep", "sp"), None)
    tok_spec = P(("rep", "sp"))
    full_spec = P(None)
    col_spec = P(None, "tp")
    wrow_spec = P("tp", None)
    cache_spec = P("rep", ("tp", "sp"), None)
    tp_swap = [(0, 1), (1, 0)]
    core_swap = [(i, i ^ 1) for i in range(sp_size)]
    chip_swap = [(i, i ^ 2) for i in range(sp_size)]

    def local_layer(x_in, positions, segments, gain_attn, w_q, w_k, w_v, w_o, gain_mlp, w_gate, w_up, w_down):
        rows_local, dim = x_in.shape
        tp_idx, sp_idx = lax.axis_index("tp"), lax.axis_index("sp")
        zeros = jnp.sum((segments == 0).astype(jnp.int32)).reshape(1)
        zeros = zeros + lax.ppermute(zeros, "sp", core_swap)
        cut = (zeros + lax.ppermute(zeros, "sp", chip_swap))[0]
        meta = jnp.stack([sp_idx, cut, tp_idx, 1 - tp_idx]).astype(jnp.int32)

        depth = w_o.shape[0]
        quarter = depth // sp_size
        wo_piece = lax.ppermute(lax.dynamic_slice(w_o, (sp_idx * quarter, 0), (quarter, dim)), "tp", tp_swap)
        wo_peer = lax.all_gather(wo_piece, "sp", tiled=True)

        cos_t, sin_t = rope_tables(positions)
        gain_a, gain_m = gain_attn.reshape(1, dim), gain_mlp.reshape(1, dim)
        u, kv_own = project_kv(x_in, gain_a, w_k, w_v, cos_t, sin_t)
        kv_core = lax.ppermute(kv_own, "sp", core_swap)
        kv_chip = lax.ppermute(kv_own, "sp", chip_swap)
        kv_diag = lax.ppermute(kv_chip, "sp", core_swap)
        kv_parts = (kv_own, kv_core, kv_chip, kv_diag)
        q_rot = project_q(u, w_q, cos_t, sin_t)

        def cache(offset):
            cols = [lax.dynamic_slice(part, (0, offset + sp_idx * HEAD_DIM), (rows_local, HEAD_DIM)) for part in kv_parts]
            odd, high = (sp_idx & 1) == 1, (sp_idx & 2) == 2
            near = jnp.concatenate([jnp.where(odd, cols[1], cols[0]), jnp.where(odd, cols[0], cols[1])], axis=0)
            far = jnp.concatenate([jnp.where(odd, cols[3], cols[2]), jnp.where(odd, cols[2], cols[3])], axis=0)
            both = jnp.concatenate([jnp.where(high, far, near), jnp.where(high, near, far)], axis=0)
            return both.reshape(sp_size * rows_local, 1, HEAD_DIM)

        chunk_rows = rows_local // CHUNKS
        attn_flops = 4 * chunk_rows * sp_size * rows_local * w_q.shape[1] // 4
        attn_mine = [attention(meta, q_rot, kv_parts, c * chunk_rows, chunk_rows, attn_flops) for c in range(CHUNKS)]
        attn_peer = [lax.ppermute(a, "tp", tp_swap) for a in attn_mine]
        k_cache, v_cache = cache(0), cache(w_k.shape[1])

        y_rows = []
        own, sums, sent = [], [], []
        for c in range(CHUNKS):
            u_mid, x_own = attn_out(meta, x_in, c, attn_mine[c], attn_peer[c], w_o, wo_peer, gain_m)
            sent.append(lax.ppermute(mlp_part(meta, 3, u_mid, w_gate, w_up, w_down), "tp", tp_swap))
            sums.append(mlp_part(meta, 2, u_mid, w_gate, w_up, w_down))
            own.append(x_own)
        first = tp_idx == 0
        for c in range(CHUNKS):
            y_own = (own[c] + (sums[c] + sent[c])).astype(BF16)
            y_peer = lax.ppermute(y_own, "tp", tp_swap)
            y_rows.append(jnp.where(first, y_own, y_peer))
            y_rows.append(jnp.where(first, y_peer, y_own))
        return jnp.concatenate(y_rows, axis=0), k_cache, v_cache

    return jax.shard_map(local_layer, mesh=mesh,
                         in_specs=(row_spec, tok_spec, tok_spec, full_spec, col_spec, col_spec, col_spec, wrow_spec,
                                   full_spec, col_spec, col_spec, wrow_spec),
                         out_specs=(row_spec, cache_spec, cache_spec), check_vma=False)
```

```python
import functools
import jax
import jax.numpy as jnp
from jax import lax
from jax.experimental import pallas as pl
from jax.experimental.pallas import tpu as pltpu
from jax.sharding import PartitionSpec as P


HEAD_DIM = 128
HALF = HEAD_DIM // 2
ROPE_BASE = 500000.0
NORM_EPS = 1e-5
LOG2E = 1.4426950408889634
BF16 = jnp.bfloat16
F32 = jnp.float32

CHUNKS = 4
Q_BLOCK = 256
K_BLOCK = 1024
FF_BLOCK = 512
MASKED = -1e30


def params(semantics, mib):
    return pltpu.CompilerParams(dimension_semantics=semantics, vmem_limit_bytes=mib << 20)


def dot(a, b):
    return jnp.dot(a, b, preferred_element_type=F32)


def normed(x, gain):
    mean_sq = jnp.mean(x * x, axis=-1, keepdims=True)
    return (x * lax.rsqrt(mean_sq + NORM_EPS) * gain).astype(BF16)


def rope_tables(positions):
    inv_freq = jnp.power(jnp.float32(ROPE_BASE), -jnp.arange(HALF, dtype=F32) * (2.0 / HEAD_DIM))
    angles = positions.astype(F32)[:, None] * inv_freq
    cos_t, sin_t = jnp.cos(angles), jnp.sin(angles)
    return jnp.concatenate([cos_t, cos_t], axis=-1), jnp.concatenate([-sin_t, sin_t], axis=-1)


def store_rotated(out_ref, rows, t_f32, cos_t, sin_t):
    for head in range(t_f32.shape[1] // HEAD_DIM):
        cols = slice(head * HEAD_DIM, (head + 1) * HEAD_DIM)
        t_head = t_f32[:, cols]
        out_ref[rows, cols] = (t_head * cos_t + pltpu.roll(t_head, HALF, 1) * sin_t).astype(BF16)


def kv_kernel(x_ref, gain_ref, wk_ref, wv_ref, cos_ref, sin_ref, u_ref, kv_ref):
    u = normed(x_ref[...].astype(F32), gain_ref[...])
    u_ref[...] = u
    width = wk_ref.shape[1]
    store_rotated(kv_ref, slice(None), dot(u, wk_ref[...]), cos_ref[...], sin_ref[...])
    kv_ref[:, width:] = dot(u, wv_ref[...]).astype(BF16)


def project_kv(x, gain, w_k, w_v, cos_t, sin_t):
    rows, dim = x.shape
    width = w_k.shape[1]
    block = 256
    whole = lambda a, b: pl.BlockSpec((a, b), lambda i: (0, 0))
    banded = lambda b: pl.BlockSpec((block, b), lambda i: (i, 0))
    return pl.pallas_call(
        kv_kernel, grid=(rows // block,), name="project_kv",
        in_specs=[banded(dim), whole(1, dim), whole(dim, width), whole(dim, width), banded(HEAD_DIM), banded(HEAD_DIM)],
        out_specs=[banded(dim), banded(2 * width)],
        out_shape=[jax.ShapeDtypeStruct((rows, dim), BF16), jax.ShapeDtypeStruct((rows, 2 * width), BF16)],
        compiler_params=params(("arbitrary",), 48),
        cost_estimate=pl.CostEstimate(flops=4 * rows * dim * width, bytes_accessed=4 * dim * (rows + width), transcendentals=0),
    )(x, gain, w_k, w_v, cos_t, sin_t)


def q_kernel(u_ref, w_ref, cos_ref, sin_ref, q_ref):
    block = 256

    @pl.loop(0, u_ref.shape[0] // block)
    def _(i):
        rows = pl.ds(pl.multiple_of(i * block, block), block)
        store_rotated(q_ref, rows, dot(u_ref[rows, :], w_ref[...]), cos_ref[rows, :], sin_ref[rows, :])


def project_q(u, w_q, cos_t, sin_t):
    rows, dim = u.shape
    width = w_q.shape[1]
    block = 512
    return pl.pallas_call(
        q_kernel, grid=(width // block,), name="project_q",
        in_specs=[pl.BlockSpec((rows, dim), lambda i: (0, 0)), pl.BlockSpec((dim, block), lambda i: (0, i)),
                  pl.BlockSpec((rows, HEAD_DIM), lambda i: (0, 0)), pl.BlockSpec((rows, HEAD_DIM), lambda i: (0, 0))],
        out_specs=pl.BlockSpec((rows, block), lambda i: (0, i)),
        out_shape=jax.ShapeDtypeStruct((rows, width), BF16),
        compiler_params=params(("arbitrary",), 48),
        cost_estimate=pl.CostEstimate(flops=2 * rows * dim * width, bytes_accessed=2 * dim * (rows + width), transcendentals=0),
    )(u, w_q, cos_t, sin_t)


def attn_kernel(group, row_base, meta_ref, q_ref, *refs):
    parts = (len(refs) - 7) // 2
    k_refs, v_refs = refs[:parts], refs[parts:2 * parts]
    o_ref, k_all, v_all, q_t, m_ref, l_ref, acc_ref = refs[2 * parts:]
    shard, cut = meta_ref[0], meta_ref[1]
    block = q_ref.shape[0]
    keys = k_refs[0].shape[0]
    scale = (HEAD_DIM ** -0.5) * LOG2E

    @pl.when(pl.program_id(1) == 0)
    def _():
        for idx in range(parts):
            rows = pl.ds(pl.multiple_of((shard ^ idx) * keys, keys), keys)
            k_all[rows, :] = k_refs[idx][...]
            v_all[:, rows] = v_refs[idx][...].T

    first = shard * keys + row_base + pl.program_id(1) * block
    last = first + block - 1
    for head in range(group):
        q_t[head] = q_ref[:, head * HEAD_DIM:(head + 1) * HEAD_DIM].T
    m_ref[...] = jnp.full_like(m_ref, MASKED)
    l_ref[...] = jnp.zeros_like(l_ref)
    acc_ref[...] = jnp.zeros_like(acc_ref)

    def step(masked, kb, carry):
        start = pl.multiple_of(kb * K_BLOCK, K_BLOCK)
        k_blk = k_all[pl.ds(start, K_BLOCK), :]
        v_blk = v_all[:, pl.ds(start, K_BLOCK)]
        scores = [dot(k_blk, q_t[head]) for head in range(group)]
        m_old = [m_ref[head] for head in range(group)]
        l_old = [l_ref[head] for head in range(group)]
        if masked:
            k_idx = start + lax.broadcasted_iota(jnp.int32, (K_BLOCK, block), 0)
            r_idx = first + lax.broadcasted_iota(jnp.int32, (K_BLOCK, block), 1)
            allowed = (k_idx <= r_idx) & ((k_idx >= cut) | (r_idx < cut))
            scores = [jnp.where(allowed, s, MASKED) for s in scores]
        news = []
        for head in range(group):
            m_new = jnp.maximum(m_old[head], jnp.max(scores[head], axis=0, keepdims=True) * scale)
            p = jnp.exp2(scores[head] * scale - m_new)
            alpha = jnp.exp2(m_old[head] - m_new)
            total = alpha * l_old[head] + jnp.sum(p, axis=0, keepdims=True)
            news.append((m_new, total, alpha, dot(v_blk, p.astype(BF16))))
        for head in range(group):
            m_ref[head], l_ref[head] = news[head][:2]
            acc_ref[head] = news[head][2] * acc_ref[head] + news[head][3]
        return carry

    low = jnp.where(first >= cut, cut, 0) // K_BLOCK
    high = last // K_BLOCK + 1
    clear = (jnp.where(last >= cut, cut, 0) + K_BLOCK - 1) // K_BLOCK
    edge_a = jnp.minimum(jnp.maximum(clear, low), high)
    edge_b = jnp.maximum(edge_a, (first + 1) // K_BLOCK)
    lax.fori_loop(edge_a, edge_b, functools.partial(step, False), 0)
    head_count = edge_a - low
    lax.fori_loop(0, head_count + high - edge_b,
                  lambda i, carry: step(True, jnp.where(i < head_count, low + i, edge_b + i - head_count), carry), 0)
    for head in range(group):
        o_ref[:, head * HEAD_DIM:(head + 1) * HEAD_DIM] = (acc_ref[head] / l_ref[head]).T.astype(BF16)


def attention(meta, q_rot, kv_parts, row_base, rows, flops):
    kv_rows, kv_width = kv_parts[0].shape
    kv_heads = kv_width // (2 * HEAD_DIM)
    group = q_rot.shape[1] // HEAD_DIM // kv_heads
    width = group * HEAD_DIM
    parts = len(kv_parts)
    base = row_base // Q_BLOCK
    k_spec = pl.BlockSpec((kv_rows, HEAD_DIM), lambda h, i, m: (0, h))
    v_spec = pl.BlockSpec((kv_rows, HEAD_DIM), lambda h, i, m: (0, kv_heads + h))
    return pl.pallas_call(
        functools.partial(attn_kernel, group, row_base), name="attention",
        grid_spec=pltpu.PrefetchScalarGridSpec(
            num_scalar_prefetch=1, grid=(kv_heads, rows // Q_BLOCK),
            in_specs=[pl.BlockSpec((Q_BLOCK, width), lambda h, i, m: (base + i, h))] + [k_spec] * parts + [v_spec] * parts,
            out_specs=pl.BlockSpec((Q_BLOCK, width), lambda h, i, m: (i, h ^ m[0])),
            scratch_shapes=[pltpu.VMEM((parts * kv_rows, HEAD_DIM), BF16), pltpu.VMEM((HEAD_DIM, parts * kv_rows), BF16),
                            pltpu.VMEM((group, HEAD_DIM, Q_BLOCK), BF16), pltpu.VMEM((group, 1, Q_BLOCK), F32),
                            pltpu.VMEM((group, 1, Q_BLOCK), F32), pltpu.VMEM((group, HEAD_DIM, Q_BLOCK), F32)]),
        out_shape=jax.ShapeDtypeStruct((rows, kv_heads * width), BF16),
        compiler_params=params(("arbitrary", "arbitrary"), 48),
        cost_estimate=pl.CostEstimate(flops=flops, bytes_accessed=16 << 20, transcendentals=0),
    )(meta, q_rot, *kv_parts, *kv_parts)


def mid_kernel(pieces, meta_ref, x_ref, a_ref, b_ref, gain_ref, *refs):
    wa_refs, wb_refs = refs[:pieces], refs[pieces:2 * pieces]
    u_ref, own_ref, mid_ref, wa_all, wb_all = refs[2 * pieces:]
    step = pl.program_id(0)
    depth, width = wa_refs[0].shape
    for idx in range(pieces):
        wa_all[idx * depth:(idx + 1) * depth, :] = wa_refs[idx][...]
        wb_all[idx * depth:(idx + 1) * depth, :] = wb_refs[idx][...]
    cols = pl.ds(pl.multiple_of(step * width, width), width)
    mid_ref[:, cols] = x_ref[...].astype(F32) + (dot(a_ref[...], wa_all[...]) + dot(b_ref[...], wb_all[...]))

    @pl.when(step == pl.num_programs(0) - 1)
    def _():
        half = own_ref.shape[0]
        own_ref[...] = mid_ref[pl.ds(pl.multiple_of(meta_ref[2] * half, half), half), :]
        block = 128

        @pl.loop(0, u_ref.shape[0] // block)
        def _(i):
            rows = pl.ds(pl.multiple_of(i * block, block), block)
            u_ref[rows, :] = normed(mid_ref[rows, :], gain_ref[...])


def attn_out(meta, x, chunk, attn_mine, attn_peer, wo_mine, wo_pieces, gain):
    rows, depth = attn_mine.shape
    dim = x.shape[1]
    block = 512
    pieces = len(wo_pieces)
    resident = lambda a, b: pl.BlockSpec((a, b), lambda i, m: (0, 0))
    mine_specs = [pl.BlockSpec((depth // pieces, block), lambda i, m, p=p: (p ^ m[0], i)) for p in range(pieces)]
    peer_specs = [pl.BlockSpec((depth // pieces, block), lambda i, m: (0, i))] * pieces
    return pl.pallas_call(
        functools.partial(mid_kernel, pieces), name="attn_out",
        grid_spec=pltpu.PrefetchScalarGridSpec(
            num_scalar_prefetch=1, grid=(dim // block,),
            in_specs=[pl.BlockSpec((rows, block), lambda i, m: (chunk, i)), resident(rows, depth), resident(rows, depth),
                      resident(1, dim)] + mine_specs + peer_specs,
            out_specs=[resident(rows, dim), resident(rows // 2, dim)],
            scratch_shapes=[pltpu.VMEM((rows, dim), F32), pltpu.VMEM((depth, block), BF16), pltpu.VMEM((depth, block), BF16)]),
        out_shape=[jax.ShapeDtypeStruct((rows, dim), BF16), jax.ShapeDtypeStruct((rows // 2, dim), F32)],
        compiler_params=params(("arbitrary",), 56),
        cost_estimate=pl.CostEstimate(flops=4 * rows * depth * dim, bytes_accessed=4 * depth * dim, transcendentals=0),
    )(meta, x, attn_mine, attn_peer, gain, *([wo_mine] * pieces), *wo_pieces)


def mlp_kernel(u_ref, wg_ref, wu_ref, wd_ref, p_ref):
    u = u_ref[...]
    gate = dot(u, wg_ref[...])
    hidden = (gate * jax.nn.sigmoid(gate) * dot(u, wu_ref[...])).astype(BF16)

    @pl.when(pl.program_id(0) == 0)
    def _():
        p_ref[...] = dot(hidden, wd_ref[...])

    @pl.when(pl.program_id(0) > 0)
    def _():
        p_ref[...] += dot(hidden, wd_ref[...])


def mlp_part(u_mid, w_gate, w_up, w_down):
    dim, ff = w_gate.shape
    rows = u_mid.shape[0]
    return pl.pallas_call(
        mlp_kernel, grid=(ff // FF_BLOCK,), name="mlp_part",
        in_specs=[pl.BlockSpec((rows, dim), lambda i: (0, 0)),
                  pl.BlockSpec((dim, FF_BLOCK), lambda i: (0, i)), pl.BlockSpec((dim, FF_BLOCK), lambda i: (0, i)),
                  pl.BlockSpec((FF_BLOCK, dim), lambda i: (i, 0))],
        out_specs=pl.BlockSpec((rows, dim), lambda i: (0, 0)),
        out_shape=jax.ShapeDtypeStruct((rows, dim), F32),
        compiler_params=params(("arbitrary",), 56),
        cost_estimate=pl.CostEstimate(flops=6 * rows * dim * ff, bytes_accessed=6 * dim * ff, transcendentals=0),
    )(u_mid, w_gate, w_up, w_down)


def solution(mesh):
    sp_size = mesh.shape["sp"]
    row_spec = P(("rep", "sp"), None)
    tok_spec = P(("rep", "sp"))
    full_spec = P(None)
    col_spec = P(None, "tp")
    wrow_spec = P("tp", None)
    cache_spec = P("rep", ("tp", "sp"), None)
    tp_swap = [(0, 1), (1, 0)]
    core_swap = [(i, i ^ 1) for i in range(sp_size)]
    chip_swap = [(i, i ^ 2) for i in range(sp_size)]

    def layer(x_in, positions, segments, gain_attn, w_q, w_k, w_v, w_o, gain_mlp, w_gate, w_up, w_down):
        rows_local, dim = x_in.shape
        tp_idx, sp_idx = lax.axis_index("tp"), lax.axis_index("sp")
        odd, high = (sp_idx & 1) == 1, (sp_idx & 2) == 2

        depth = w_o.shape[0]
        quarter = depth // sp_size
        wo_own = lax.ppermute(lax.dynamic_slice(w_o, (sp_idx * quarter, 0), (quarter, dim)), "tp", tp_swap)

        zeros = jnp.sum((segments == 0).astype(jnp.int32)).reshape(1)
        zeros = zeros + lax.ppermute(zeros, "sp", core_swap)
        cut = (zeros + lax.ppermute(zeros, "sp", chip_swap))[0]
        meta = jnp.stack([sp_idx, cut, tp_idx, 1 - tp_idx]).astype(jnp.int32)

        cos_t, sin_t = rope_tables(positions)
        gain_a, gain_m = gain_attn.reshape(1, dim), gain_mlp.reshape(1, dim)
        u, kv_own = project_kv(x_in, gain_a, w_k, w_v, cos_t, sin_t)
        kv_chip = lax.ppermute(kv_own, "sp", chip_swap)
        kv_core = lax.ppermute(kv_own, "sp", core_swap)
        kv_diag = lax.ppermute(kv_chip, "sp", core_swap)
        kv_parts = (kv_own, kv_core, kv_chip, kv_diag)
        q_rot = project_q(u, w_q, cos_t, sin_t)

        wo_chip = lax.ppermute(wo_own, "sp", chip_swap)
        wo_core = lax.ppermute(wo_own, "sp", core_swap)
        wo_diag = lax.ppermute(wo_chip, "sp", core_swap)
        wo_pieces = (wo_own, wo_core, wo_chip, wo_diag)

        def ordered(own, core, chip, diag):
            near = jnp.concatenate([jnp.where(odd, core, own), jnp.where(odd, own, core)], axis=0)
            far = jnp.concatenate([jnp.where(odd, diag, chip), jnp.where(odd, chip, diag)], axis=0)
            return jnp.concatenate([jnp.where(high, far, near), jnp.where(high, near, far)], axis=0)

        def cache(offset):
            cols = [lax.dynamic_slice(part, (0, offset + sp_idx * HEAD_DIM), (rows_local, HEAD_DIM)) for part in kv_parts]
            return ordered(*cols).reshape(sp_size * rows_local, 1, HEAD_DIM)

        chunk_rows = rows_local // CHUNKS
        half = chunk_rows // 2
        attn_flops = 4 * chunk_rows * sp_size * rows_local * w_q.shape[1] // 4
        attn_mine, attn_peer = [], []
        for c in range(CHUNKS):
            attn_mine.append(attention(meta, q_rot, kv_parts, c * chunk_rows, chunk_rows, attn_flops))
            attn_peer.append(lax.ppermute(attn_mine[c], "tp", tp_swap))
        k_cache, v_cache = cache(0), cache(w_k.shape[1])
        y_out = jnp.zeros((rows_local, dim), BF16)
        k_cache, v_cache, y_out, attn_peer[0] = lax.optimization_barrier((k_cache, v_cache, y_out, attn_peer[0]))

        own, sums, sent = [], [], []
        for c in range(CHUNKS):
            u_mid, x_own = attn_out(meta, x_in, c, attn_mine[c], attn_peer[c], w_o, wo_pieces, gain_m)
            p_sum = mlp_part(u_mid, w_gate, w_up, w_down)
            sent.append(lax.ppermute(lax.dynamic_slice(p_sum, ((1 - tp_idx) * half, 0), (half, dim)), "tp", tp_swap))
            sums.append(lax.dynamic_slice(p_sum, (tp_idx * half, 0), (half, dim)))
            own.append(x_own)
        for c in range(CHUNKS):
            y_own = lax.optimization_barrier((own[c] + (sums[c] + sent[c])).astype(BF16))
            y_peer = lax.ppermute(y_own, "tp", tp_swap)
            y_out = lax.dynamic_update_slice(y_out, y_own, (c * chunk_rows + tp_idx * half, 0))
            y_out = lax.dynamic_update_slice(y_out, y_peer, (c * chunk_rows + (1 - tp_idx) * half, 0))
        return y_out, k_cache, v_cache


    return jax.shard_map(layer, mesh=mesh,
                         in_specs=(row_spec, tok_spec, tok_spec, full_spec, col_spec, col_spec, col_spec, wrow_spec,
                                   full_spec, col_spec, col_spec, wrow_spec),
                         out_specs=(row_spec, cache_spec, cache_spec), check_vma=False)
```

```python
import functools
import jax
import jax.numpy as jnp
from jax import lax
from jax.experimental import pallas as pl
from jax.experimental.pallas import tpu as pltpu
from jax.sharding import PartitionSpec as P


HEAD_DIM = 128
HALF = HEAD_DIM // 2
ROPE_BASE = 500000.0
NORM_EPS = 1e-5
LOG2E = 1.4426950408889634
BF16 = jnp.bfloat16
F32 = jnp.float32

CHUNKS = 4
Q_BLOCK = 256
K_BLOCK = 1024
FF_BLOCK = 512
MASKED = -1e30


def params(semantics, mib):
    return pltpu.CompilerParams(dimension_semantics=semantics, vmem_limit_bytes=mib << 20)


def dot(a, b):
    return jnp.dot(a, b, preferred_element_type=F32)


def normed(x, gain):
    mean_sq = jnp.mean(x * x, axis=-1, keepdims=True)
    return (x * lax.rsqrt(mean_sq + NORM_EPS) * gain).astype(BF16)


def rope_tables(positions):
    inv_freq = jnp.power(jnp.float32(ROPE_BASE), -jnp.arange(HALF, dtype=F32) * (2.0 / HEAD_DIM))
    angles = positions.astype(F32)[:, None] * jnp.concatenate([inv_freq, inv_freq])
    sign = jnp.where(jnp.arange(HEAD_DIM) < HALF, -1.0, 1.0).astype(F32)
    return jnp.cos(angles), jnp.sin(angles) * sign


def store_rotated(out_ref, rows, t_f32, cos_t, sin_t):
    for head in range(t_f32.shape[1] // HEAD_DIM):
        cols = slice(head * HEAD_DIM, (head + 1) * HEAD_DIM)
        t_head = t_f32[:, cols]
        out_ref[rows, cols] = (t_head * cos_t + pltpu.roll(t_head, HALF, 1) * sin_t).astype(BF16)


def kv_kernel(x_ref, gain_ref, wk_ref, wv_ref, cos_ref, sin_ref, u_ref, kv_ref):
    u = normed(x_ref[...].astype(F32), gain_ref[...])
    u_ref[...] = u
    width = wk_ref.shape[1]
    store_rotated(kv_ref, slice(None), dot(u, wk_ref[...]), cos_ref[...], sin_ref[...])
    kv_ref[:, width:] = dot(u, wv_ref[...]).astype(BF16)


def project_kv(x, gain, w_k, w_v, cos_t, sin_t):
    rows, dim = x.shape
    width = w_k.shape[1]
    block = 256
    whole = lambda a, b: pl.BlockSpec((a, b), lambda i: (0, 0))
    banded = lambda b: pl.BlockSpec((block, b), lambda i: (i, 0))
    return pl.pallas_call(
        kv_kernel, grid=(rows // block,), name="project_kv",
        in_specs=[banded(dim), whole(1, dim), whole(dim, width), whole(dim, width), banded(HEAD_DIM), banded(HEAD_DIM)],
        out_specs=[banded(dim), banded(2 * width)],
        out_shape=[jax.ShapeDtypeStruct((rows, dim), BF16), jax.ShapeDtypeStruct((rows, 2 * width), BF16)],
        compiler_params=params(("arbitrary",), 48),
        cost_estimate=pl.CostEstimate(flops=4 * rows * dim * width, bytes_accessed=4 * dim * (rows + width), transcendentals=0),
    )(x, gain, w_k, w_v, cos_t, sin_t)


def q_kernel(u_ref, w_ref, cos_ref, sin_ref, q_ref):
    block = 512

    @pl.loop(0, u_ref.shape[0] // block)
    def _(i):
        rows = pl.ds(pl.multiple_of(i * block, block), block)
        store_rotated(q_ref, rows, dot(u_ref[rows, :], w_ref[...]), cos_ref[rows, :], sin_ref[rows, :])


def project_q(u, w_q, cos_t, sin_t):
    rows, dim = u.shape
    width = w_q.shape[1]
    block = 512
    return pl.pallas_call(
        q_kernel, grid=(width // block,), name="project_q",
        in_specs=[pl.BlockSpec((rows, dim), lambda i: (0, 0)), pl.BlockSpec((dim, block), lambda i: (0, i)),
                  pl.BlockSpec((rows, HEAD_DIM), lambda i: (0, 0)), pl.BlockSpec((rows, HEAD_DIM), lambda i: (0, 0))],
        out_specs=pl.BlockSpec((rows, block), lambda i: (0, i)),
        out_shape=jax.ShapeDtypeStruct((rows, width), BF16),
        compiler_params=params(("arbitrary",), 48),
        cost_estimate=pl.CostEstimate(flops=2 * rows * dim * width, bytes_accessed=2 * dim * (rows + width), transcendentals=0),
    )(u, w_q, cos_t, sin_t)


def attn_kernel(group, row_base, finish, meta_ref, q_ref, *refs):
    k_refs, v_refs = refs[:2], refs[2:4]
    if finish:
        acc_in, m_in, l_in, o_ref = refs[4:8]
    else:
        acc_out, m_out, l_out = refs[4:7]
    k_all, v_all, q_t, m_ref, l_ref, acc_ref = refs[-6:]
    shard, cut = meta_ref[0], meta_ref[1]
    block = q_ref.shape[0]
    keys = k_refs[0].shape[0]
    scale = (HEAD_DIM ** -0.5) * LOG2E
    chip_base = (shard // 2) * (2 * keys)
    base = 0 if finish else chip_base

    @pl.when(pl.program_id(1) == 0)
    def _():
        for idx in range(2):
            rows = pl.ds(pl.multiple_of(((shard ^ idx) & 1) * keys, keys), keys)
            k_all[rows, :] = k_refs[idx][...]
            v_all[:, rows] = v_refs[idx][...].T

    first = shard * keys + row_base + pl.program_id(1) * block
    last = first + block - 1
    for head in range(group):
        q_t[head] = q_ref[:, head * HEAD_DIM:(head + 1) * HEAD_DIM].T
    if finish:
        m_ref[...], l_ref[...], acc_ref[...] = m_in[...], l_in[...], acc_in[...]
    else:
        m_ref[...] = jnp.full_like(m_ref, MASKED)
        l_ref[...] = jnp.zeros_like(l_ref)
        acc_ref[...] = jnp.zeros_like(acc_ref)

    def step(masked, kb, carry):
        start = kb * K_BLOCK
        rows = pl.ds(pl.multiple_of(start - base, K_BLOCK), K_BLOCK)
        k_blk = k_all[rows, :]
        v_blk = v_all[:, rows]
        scores = [dot(k_blk, q_t[head]) for head in range(group)]
        m_old = [m_ref[head] for head in range(group)]
        l_old = [l_ref[head] for head in range(group)]
        if masked:
            k_idx = start + lax.broadcasted_iota(jnp.int32, (K_BLOCK, block), 0)
            r_idx = first + lax.broadcasted_iota(jnp.int32, (K_BLOCK, block), 1)
            allowed = (k_idx <= r_idx) & ((k_idx >= cut) | (r_idx < cut))
            scores = [jnp.where(allowed, s, MASKED) for s in scores]
        news = []
        for head in range(group):
            m_new = jnp.maximum(m_old[head], jnp.max(scores[head], axis=0, keepdims=True) * scale)
            p = jnp.exp2(scores[head] * scale - m_new)
            alpha = jnp.exp2(m_old[head] - m_new)
            total = alpha * l_old[head] + jnp.sum(p, axis=0, keepdims=True)
            news.append((m_new, total, alpha, dot(v_blk, p.astype(BF16))))
        for head in range(group):
            m_ref[head], l_ref[head] = news[head][:2]
            acc_ref[head] = news[head][2] * acc_ref[head] + news[head][3]
        return carry

    seg_low = jnp.where(first >= cut, cut, 0)
    seg_high = jnp.where(last >= cut, cut, 0)
    low = jnp.maximum(seg_low, base) // K_BLOCK
    high = chip_base // K_BLOCK if finish else last // K_BLOCK + 1
    clear = (seg_high + K_BLOCK - 1) // K_BLOCK
    edge_a = jnp.maximum(low, jnp.minimum(clear, high))
    edge_b = jnp.maximum(edge_a, jnp.minimum((first + 1) // K_BLOCK, high))
    head_count = edge_a - low
    lax.fori_loop(edge_a, edge_b, functools.partial(step, False), 0)
    lax.fori_loop(0, head_count + jnp.maximum(high - edge_b, 0),
                  lambda i, carry: step(True, jnp.where(i < head_count, low + i, edge_b + i - head_count), carry), 0)
    if finish:
        for head in range(group):
            o_ref[:, head * HEAD_DIM:(head + 1) * HEAD_DIM] = (acc_ref[head] / l_ref[head]).T.astype(BF16)
    else:
        acc_out[...], m_out[...], l_out[...] = acc_ref[...], m_ref[...], l_ref[...]


def attention(meta, q_rot, kv_parts, row_base, rows, flops, partial_sums=None):
    kv_rows, kv_width = kv_parts[0].shape
    kv_heads = kv_width // (2 * HEAD_DIM)
    group = q_rot.shape[1] // HEAD_DIM // kv_heads
    width = group * HEAD_DIM
    base = row_base // Q_BLOCK
    finish = partial_sums is not None
    k_spec = pl.BlockSpec((kv_rows, HEAD_DIM), lambda h, i, m: (0, h))
    v_spec = pl.BlockSpec((kv_rows, HEAD_DIM), lambda h, i, m: (0, kv_heads + h))
    sums_specs = [pl.BlockSpec((group, depth, Q_BLOCK), lambda h, i, m: (h, 0, base + i)) for depth in (HEAD_DIM, 1, 1)]
    sums_shapes = [jax.ShapeDtypeStruct((kv_heads * group, depth, rows), F32) for depth in (HEAD_DIM, 1, 1)]
    return pl.pallas_call(
        functools.partial(attn_kernel, group, row_base, finish), name="attention",
        grid_spec=pltpu.PrefetchScalarGridSpec(
            num_scalar_prefetch=1, grid=(kv_heads, rows // Q_BLOCK),
            in_specs=[pl.BlockSpec((Q_BLOCK, width), lambda h, i, m: (base + i, h)), k_spec, k_spec, v_spec, v_spec]
                     + (sums_specs if finish else []),
            out_specs=pl.BlockSpec((Q_BLOCK, width), lambda h, i, m: (i, h ^ m[0])) if finish else sums_specs,
            scratch_shapes=[pltpu.VMEM((2 * kv_rows, HEAD_DIM), BF16), pltpu.VMEM((HEAD_DIM, 2 * kv_rows), BF16),
                            pltpu.VMEM((group, HEAD_DIM, Q_BLOCK), BF16), pltpu.VMEM((group, 1, Q_BLOCK), F32),
                            pltpu.VMEM((group, 1, Q_BLOCK), F32), pltpu.VMEM((group, HEAD_DIM, Q_BLOCK), F32)]),
        out_shape=jax.ShapeDtypeStruct((rows, kv_heads * width), BF16) if finish else sums_shapes,
        compiler_params=params(("arbitrary", "arbitrary"), 48),
        cost_estimate=pl.CostEstimate(flops=flops, bytes_accessed=16 << 20, transcendentals=0),
    )(meta, q_rot, *kv_parts, *kv_parts, *(partial_sums or ()))


def chunk_kernel(mine, peer, out_steps, meta_ref, x_ref, a_ref, b_ref, gain_ref, *refs):
    wa_refs, wb_refs = refs[:mine], refs[mine:mine + peer]
    wg_ref, wu_ref, wd_ref, send_ref, keep_ref, mid_ref, u_ref, acc_ref, wa_all, wb_all = refs[mine + peer:]
    step = pl.program_id(0)
    half = send_ref.shape[0]
    own = pl.ds(pl.multiple_of(meta_ref[2] * half, half), half)
    other = pl.ds(pl.multiple_of(meta_ref[3] * half, half), half)

    @pl.when(step < out_steps)
    def _():
        width = wa_all.shape[1]
        for pieces, whole in ((wa_refs, wa_all), (wb_refs, wb_all)):
            top = 0
            for piece in pieces:
                whole[top:top + piece.shape[0], :] = piece[...]
                top += piece.shape[0]
        cols = pl.ds(pl.multiple_of(step * width, width), width)
        mid_ref[:, cols] = x_ref[...].astype(F32) + (dot(a_ref[...], wa_all[...]) + dot(b_ref[...], wb_all[...]))

    @pl.when(step == out_steps - 1)
    def _():
        u_ref[:half, :] = normed(mid_ref[other, :], gain_ref[...])
        u_ref[half:, :] = normed(mid_ref[own, :], gain_ref[...])
        acc_ref[...] = jnp.zeros_like(acc_ref)

    @pl.when(step >= out_steps)
    def _():
        u = u_ref[...]
        gate = dot(u, wg_ref[...])
        hidden = (gate * jax.nn.sigmoid(gate) * dot(u, wu_ref[...])).astype(BF16)
        acc_ref[...] += dot(hidden, wd_ref[...])

    @pl.when(step == pl.num_programs(0) - 1)
    def _():
        send_ref[...] = acc_ref[:half, :]
        keep_ref[...] = mid_ref[own, :] + acc_ref[half:, :]


def chunk_layer(meta, x, chunk, attn_mine, attn_peer, wo_mine, wo_pieces, gain, w_gate, w_up, w_down):
    rows, depth = attn_mine.shape
    dim, ff = w_gate.shape
    block = 512
    out_steps, mlp_steps = dim // block, ff // FF_BLOCK
    heads = 4
    resident = lambda a, b: pl.BlockSpec((a, b), lambda i, m: (0, 0))
    early = lambda i: jnp.minimum(i, out_steps - 1)
    late = lambda i: jnp.maximum(i - out_steps, 0)
    mine_specs = [pl.BlockSpec((depth // heads, block), lambda i, m, p=p: (p ^ m[0], early(i))) for p in range(heads)]
    peer_specs = [pl.BlockSpec((w.shape[0], block), lambda i, m: (0, early(i))) for w in wo_pieces]
    return pl.pallas_call(
        functools.partial(chunk_kernel, heads, len(wo_pieces), out_steps), name="chunk_layer",
        grid_spec=pltpu.PrefetchScalarGridSpec(
            num_scalar_prefetch=1, grid=(out_steps + mlp_steps,),
            in_specs=[pl.BlockSpec((rows, block), lambda i, m: (chunk, early(i))), resident(rows, depth), resident(rows, depth),
                      resident(1, dim)] + mine_specs + peer_specs
                     + [pl.BlockSpec((dim, FF_BLOCK), lambda i, m: (0, late(i))), pl.BlockSpec((dim, FF_BLOCK), lambda i, m: (0, late(i))),
                        pl.BlockSpec((FF_BLOCK, dim), lambda i, m: (late(i), 0))],
            out_specs=[resident(rows // 2, dim)] * 2,
            scratch_shapes=[pltpu.VMEM((rows, dim), F32), pltpu.VMEM((rows, dim), BF16), pltpu.VMEM((rows, dim), F32),
                            pltpu.VMEM((depth, block), BF16), pltpu.VMEM((depth, block), BF16)]),
        out_shape=[jax.ShapeDtypeStruct((rows // 2, dim), F32)] * 2,
        compiler_params=params(("arbitrary",), 60),
        cost_estimate=pl.CostEstimate(flops=4 * rows * depth * dim + 6 * rows * dim * ff, bytes_accessed=6 * dim * ff, transcendentals=0),
    )(meta, x, attn_mine, attn_peer, gain, *([wo_mine] * heads), *wo_pieces, w_gate, w_up, w_down)


def solution(mesh):
    sp_size = mesh.shape["sp"]
    row_spec = P(("rep", "sp"), None)
    tok_spec = P(("rep", "sp"))
    full_spec = P(None)
    col_spec = P(None, "tp")
    wrow_spec = P("tp", None)
    cache_spec = P("rep", ("tp", "sp"), None)
    tp_swap = [(0, 1), (1, 0)]
    core_swap = [(i, i ^ 1) for i in range(sp_size)]
    chip_swap = [(i, i ^ 2) for i in range(sp_size)]

    def layer(x_in, positions, segments, gain_attn, w_q, w_k, w_v, w_o, gain_mlp, w_gate, w_up, w_down):
        rows_local, dim = x_in.shape
        tp_idx, sp_idx = lax.axis_index("tp"), lax.axis_index("sp")
        odd, high = (sp_idx & 1) == 1, (sp_idx & 2) == 2

        depth = w_o.shape[0]
        quarter = depth // sp_size
        half_q = quarter // 2
        wo_own = lax.ppermute(lax.dynamic_slice(w_o, (sp_idx * quarter, 0), (quarter, dim)), "tp", tp_swap)
        wo_far = lax.ppermute(lax.dynamic_slice(w_o, ((sp_idx ^ 2) * quarter, 0), (half_q, dim)), "tp", tp_swap)

        zeros = jnp.sum((segments == 0).astype(jnp.int32)).reshape(1)
        zeros = zeros + lax.ppermute(zeros, "sp", core_swap)
        cut = (zeros + lax.ppermute(zeros, "sp", chip_swap))[0]
        meta = jnp.stack([sp_idx, cut, tp_idx, 1 - tp_idx]).astype(jnp.int32)

        cos_t, sin_t = rope_tables(positions)
        gain_a, gain_m = gain_attn.reshape(1, dim), gain_mlp.reshape(1, dim)
        u, kv_own = project_kv(x_in, gain_a, w_k, w_v, cos_t, sin_t)
        kv_chip = lax.ppermute(kv_own, "sp", chip_swap)
        kv_core = lax.ppermute(kv_own, "sp", core_swap)
        kv_diag = lax.ppermute(kv_chip, "sp", core_swap)
        kv_parts = (kv_own, kv_core, kv_chip, kv_diag)
        q_rot = project_q(u, w_q, cos_t, sin_t)

        wo_near = lax.ppermute(wo_own[half_q:], "sp", chip_swap)
        wo_core = lax.ppermute(wo_own, "sp", core_swap)
        wo_dfar = lax.ppermute(wo_far, "sp", core_swap)
        wo_dnear = lax.ppermute(wo_near, "sp", core_swap)
        wo_pieces = (wo_own, wo_core, wo_far, wo_near, wo_dfar, wo_dnear)

        def ordered(own, core, chip, diag):
            near = jnp.concatenate([jnp.where(odd, core, own), jnp.where(odd, own, core)], axis=0)
            far = jnp.concatenate([jnp.where(odd, diag, chip), jnp.where(odd, chip, diag)], axis=0)
            return jnp.concatenate([jnp.where(high, far, near), jnp.where(high, near, far)], axis=0)

        def cache(offset):
            cols = [lax.dynamic_slice(part, (0, offset + sp_idx * HEAD_DIM), (rows_local, HEAD_DIM)) for part in kv_parts]
            return ordered(*cols).reshape(sp_size * rows_local, 1, HEAD_DIM)

        chunk_rows = rows_local // CHUNKS
        half = chunk_rows // 2
        attn_flops = 4 * chunk_rows * sp_size * rows_local * w_q.shape[1] // 4
        partial_sums = attention(meta, q_rot, kv_parts[:2], 0, rows_local, attn_flops)
        attn_mine, attn_peer = [], []
        for c in range(CHUNKS):
            attn_mine.append(attention(meta, q_rot, kv_parts[2:], c * chunk_rows, chunk_rows, attn_flops, partial_sums))
            attn_peer.append(lax.ppermute(attn_mine[c], "tp", tp_swap))
        k_cache, v_cache = cache(0), cache(w_k.shape[1])
        y_out = jnp.zeros((rows_local, dim), BF16)
        k_cache, v_cache, y_out, attn_peer[0] = lax.optimization_barrier((k_cache, v_cache, y_out, attn_peer[0]))

        kept, sent = [], []
        for c in range(CHUNKS):
            p_peer, p_own = chunk_layer(meta, x_in, c, attn_mine[c], attn_peer[c], w_o, wo_pieces, gain_m,
                                   w_gate, w_up, w_down)
            sent.append(lax.ppermute(p_peer, "tp", tp_swap))
            kept.append(p_own)
        for c in range(CHUNKS):
            y_own = lax.optimization_barrier((kept[c] + sent[c]).astype(BF16))
            y_peer = lax.ppermute(y_own, "tp", tp_swap)
            y_out = lax.dynamic_update_slice(y_out, y_own, (c * chunk_rows + tp_idx * half, 0))
            y_out = lax.dynamic_update_slice(y_out, y_peer, (c * chunk_rows + (1 - tp_idx) * half, 0))
        return y_out, k_cache, v_cache


    return jax.shard_map(layer, mesh=mesh,
                         in_specs=(row_spec, tok_spec, tok_spec, full_spec, col_spec, col_spec, col_spec, wrow_spec,
                                   full_spec, col_spec, col_spec, wrow_spec),
                         out_specs=(row_spec, cache_spec, cache_spec), check_vma=False)
```

```python
import functools
import jax
import jax.numpy as jnp
from jax import lax
from jax.experimental import pallas as pl
from jax.experimental.pallas import tpu as pltpu
from jax.sharding import PartitionSpec as P


HEAD_DIM = 128
HALF = HEAD_DIM // 2
ROPE_BASE = 500000.0
NORM_EPS = 1e-5
LOG2E = 1.4426950408889634
BF16 = jnp.bfloat16
F32 = jnp.float32

CHUNKS = 4
Q_BLOCK = 256
FF_BLOCK = 512
MASKED = -1e30


def params(semantics, mib):
    return pltpu.CompilerParams(dimension_semantics=semantics, vmem_limit_bytes=mib << 20)


def dot(a, b):
    return jnp.dot(a, b, preferred_element_type=F32)


def normed(x, gain):
    mean_sq = jnp.mean(x * x, axis=-1, keepdims=True)
    return (x * lax.rsqrt(mean_sq + NORM_EPS) * gain).astype(BF16)


def rope_tables(positions):
    inv_freq = jnp.power(jnp.float32(ROPE_BASE), -jnp.arange(HALF, dtype=F32) * (2.0 / HEAD_DIM))
    angles = positions.astype(F32)[:, None] * jnp.concatenate([inv_freq, inv_freq])
    sign = jnp.where(jnp.arange(HEAD_DIM) < HALF, -1.0, 1.0).astype(F32)
    return jnp.cos(angles), jnp.sin(angles) * sign


def store_rotated(out_ref, rows, t_f32, cos_t, sin_t):
    for head in range(t_f32.shape[1] // HEAD_DIM):
        cols = slice(head * HEAD_DIM, (head + 1) * HEAD_DIM)
        t_head = t_f32[:, cols]
        out_ref[rows, cols] = (t_head * cos_t + pltpu.roll(t_head, HALF, 1) * sin_t).astype(BF16)


def kv_kernel(x_ref, gain_ref, wk_ref, wv_ref, cos_ref, sin_ref, u_ref, kv_ref):
    u = normed(x_ref[...].astype(F32), gain_ref[...])
    u_ref[...] = u
    width = wk_ref.shape[1]
    store_rotated(kv_ref, slice(None), dot(u, wk_ref[...]), cos_ref[...], sin_ref[...])
    kv_ref[:, width:] = dot(u, wv_ref[...]).astype(BF16)


def project_kv(x, gain, w_k, w_v, cos_t, sin_t):
    rows, dim = x.shape
    width = w_k.shape[1]
    block = 256
    whole = lambda a, b: pl.BlockSpec((a, b), lambda i: (0, 0))
    banded = lambda b: pl.BlockSpec((block, b), lambda i: (i, 0))
    return pl.pallas_call(
        kv_kernel, grid=(rows // block,), name="project_kv",
        in_specs=[banded(dim), whole(1, dim), whole(dim, width), whole(dim, width), banded(HEAD_DIM), banded(HEAD_DIM)],
        out_specs=[banded(dim), banded(2 * width)],
        out_shape=[jax.ShapeDtypeStruct((rows, dim), BF16), jax.ShapeDtypeStruct((rows, 2 * width), BF16)],
        compiler_params=params(("arbitrary",), 48),
        cost_estimate=pl.CostEstimate(flops=4 * rows * dim * width, bytes_accessed=4 * dim * (rows + width), transcendentals=0),
    )(x, gain, w_k, w_v, cos_t, sin_t)


def q_kernel(u_ref, w_ref, cos_ref, sin_ref, q_ref):
    block = 512

    @pl.loop(0, u_ref.shape[0] // block)
    def _(i):
        rows = pl.ds(pl.multiple_of(i * block, block), block)
        store_rotated(q_ref, rows, dot(u_ref[rows, :], w_ref[...]), cos_ref[rows, :], sin_ref[rows, :])


def project_q(u, w_q, cos_t, sin_t):
    rows, dim = u.shape
    width = w_q.shape[1]
    block = 512
    return pl.pallas_call(
        q_kernel, grid=(width // block,), name="project_q",
        in_specs=[pl.BlockSpec((rows, dim), lambda i: (0, 0)), pl.BlockSpec((dim, block), lambda i: (0, i)),
                  pl.BlockSpec((rows, HEAD_DIM), lambda i: (0, 0)), pl.BlockSpec((rows, HEAD_DIM), lambda i: (0, 0))],
        out_specs=pl.BlockSpec((rows, block), lambda i: (0, i)),
        out_shape=jax.ShapeDtypeStruct((rows, width), BF16),
        compiler_params=params(("arbitrary",), 48),
        cost_estimate=pl.CostEstimate(flops=2 * rows * dim * width, bytes_accessed=2 * dim * (rows + width), transcendentals=0),
    )(u, w_q, cos_t, sin_t)


def attn_kernel(group, row_base, parts, k_block, load, finish, meta_ref, q_ref, *refs):
    k_refs, v_refs, refs = refs[:parts], refs[parts:2 * parts], refs[2 * parts:]
    if load:
        acc_in, m_in, l_in = refs[:3]
    if finish:
        o_ref = refs[-7]
    else:
        acc_out, m_out, l_out = refs[:3]
    k_all, v_all, q_t, m_ref, l_ref, acc_ref = refs[-6:]
    shard, cut = meta_ref[0], meta_ref[1]
    block = q_ref.shape[0]
    keys = k_refs[0].shape[0]
    scale = (HEAD_DIM ** -0.5) * LOG2E
    chip_base = (shard // 2) * (2 * keys)
    base = 0 if finish else chip_base

    @pl.when(pl.program_id(1) == 0)
    def _():
        for idx in range(parts):
            rows = pl.ds(pl.multiple_of(((shard ^ idx) & (parts - 1)) * keys, keys), keys)
            k_all[rows, :] = k_refs[idx][...]
            v_all[:, rows] = v_refs[idx][...].T

    first = shard * keys + row_base + pl.program_id(1) * block
    last = first + block - 1
    for head in range(group):
        q_t[head] = q_ref[:, head * HEAD_DIM:(head + 1) * HEAD_DIM].T
    if load:
        m_ref[...], l_ref[...], acc_ref[...] = m_in[...], l_in[...], acc_in[...]
    else:
        m_ref[...] = jnp.full_like(m_ref, MASKED)
        l_ref[...] = jnp.zeros_like(l_ref)
        acc_ref[...] = jnp.zeros_like(acc_ref)

    def step(masked, kb, carry):
        start = kb * k_block
        rows = pl.ds(pl.multiple_of(start - base, k_block), k_block)
        k_blk = k_all[rows, :]
        v_blk = v_all[:, rows]
        scores = [dot(k_blk, q_t[head]) for head in range(group)]
        m_old = [m_ref[head] for head in range(group)]
        l_old = [l_ref[head] for head in range(group)]
        if masked:
            k_idx = start + lax.broadcasted_iota(jnp.int32, (k_block, block), 0)
            r_idx = first + lax.broadcasted_iota(jnp.int32, (k_block, block), 1)
            allowed = (k_idx <= r_idx) & ((k_idx >= cut) | (r_idx < cut))
            scores = [jnp.where(allowed, s, MASKED) for s in scores]
        news = []
        for head in range(group):
            m_new = jnp.maximum(m_old[head], jnp.max(scores[head], axis=0, keepdims=True) * scale)
            p = jnp.exp2(scores[head] * scale - m_new)
            alpha = jnp.exp2(m_old[head] - m_new)
            total = alpha * l_old[head] + jnp.sum(p, axis=0, keepdims=True)
            news.append((m_new, total, alpha, dot(v_blk, p.astype(BF16))))
        for head in range(group):
            m_ref[head], l_ref[head] = news[head][:2]
            acc_ref[head] = news[head][2] * acc_ref[head] + news[head][3]
        return carry

    seg_low = jnp.where(first >= cut, cut, 0)
    seg_high = jnp.where(last >= cut, cut, 0)
    low = jnp.maximum(seg_low, base) // k_block
    high = chip_base // k_block if load else last // k_block + 1
    clear = (seg_high + k_block - 1) // k_block
    edge_a = jnp.maximum(low, jnp.minimum(clear, high))
    edge_b = jnp.maximum(edge_a, jnp.minimum((first + 1) // k_block, high))
    head_count = edge_a - low
    lax.fori_loop(edge_a, edge_b, functools.partial(step, False), 0)
    lax.fori_loop(0, head_count + jnp.maximum(high - edge_b, 0),
                  lambda i, carry: step(True, jnp.where(i < head_count, low + i, edge_b + i - head_count), carry), 0)
    if finish:
        for head in range(group):
            o_ref[:, head * HEAD_DIM:(head + 1) * HEAD_DIM] = (acc_ref[head] / l_ref[head]).T.astype(BF16)
    else:
        acc_out[...], m_out[...], l_out[...] = acc_ref[...], m_ref[...], l_ref[...]


def attention(meta, q_rot, kv_parts, row_base, rows, k_block, flops, finish=True, partial_sums=None):
    kv_rows, kv_width = kv_parts[0].shape
    kv_heads = kv_width // (2 * HEAD_DIM)
    group = q_rot.shape[1] // HEAD_DIM // kv_heads
    width = group * HEAD_DIM
    base = row_base // Q_BLOCK
    parts, load = len(kv_parts), partial_sums is not None
    k_spec = pl.BlockSpec((kv_rows, HEAD_DIM), lambda h, i, m: (0, h))
    v_spec = pl.BlockSpec((kv_rows, HEAD_DIM), lambda h, i, m: (0, kv_heads + h))
    sums_specs = [pl.BlockSpec((group, depth, Q_BLOCK), lambda h, i, m: (h, 0, base + i)) for depth in (HEAD_DIM, 1, 1)]
    sums_shapes = [jax.ShapeDtypeStruct((kv_heads * group, depth, rows), F32) for depth in (HEAD_DIM, 1, 1)]
    return pl.pallas_call(
        functools.partial(attn_kernel, group, row_base, parts, k_block, load, finish), name="attention",
        grid_spec=pltpu.PrefetchScalarGridSpec(
            num_scalar_prefetch=1, grid=(kv_heads, rows // Q_BLOCK),
            in_specs=[pl.BlockSpec((Q_BLOCK, width), lambda h, i, m: (base + i, h))] + [k_spec] * parts + [v_spec] * parts
                     + (sums_specs if load else []),
            out_specs=pl.BlockSpec((Q_BLOCK, width), lambda h, i, m: (i, h ^ m[0])) if finish else sums_specs,
            scratch_shapes=[pltpu.VMEM((parts * kv_rows, HEAD_DIM), BF16), pltpu.VMEM((HEAD_DIM, parts * kv_rows), BF16),
                            pltpu.VMEM((group, HEAD_DIM, Q_BLOCK), BF16), pltpu.VMEM((group, 1, Q_BLOCK), F32),
                            pltpu.VMEM((group, 1, Q_BLOCK), F32), pltpu.VMEM((group, HEAD_DIM, Q_BLOCK), F32)]),
        out_shape=jax.ShapeDtypeStruct((rows, kv_heads * width), BF16) if finish else sums_shapes,
        compiler_params=params(("arbitrary", "arbitrary"), 48),
        cost_estimate=pl.CostEstimate(flops=flops, bytes_accessed=16 << 20, transcendentals=0),
    )(meta, q_rot, *kv_parts, *kv_parts, *(partial_sums or ()))


def chunk_kernel(mine, peer, out_steps, meta_ref, x_ref, a_ref, b_ref, gain_ref, *refs):
    wa_refs, wb_refs = refs[:mine], refs[mine:mine + peer]
    wg_ref, wu_ref, wd_ref, send_ref, keep_ref, mid_ref, u_ref, acc_ref, wa_all, wb_all = refs[mine + peer:]
    step = pl.program_id(0)
    half = send_ref.shape[0]
    own = pl.ds(pl.multiple_of(meta_ref[2] * half, half), half)
    other = pl.ds(pl.multiple_of(meta_ref[3] * half, half), half)

    @pl.when(step < out_steps)
    def _():
        width = wa_all.shape[1]
        for pieces, whole in ((wa_refs, wa_all), (wb_refs, wb_all)):
            top = 0
            for piece in pieces:
                whole[top:top + piece.shape[0], :] = piece[...]
                top += piece.shape[0]
        cols = pl.ds(pl.multiple_of(step * width, width), width)
        mid_ref[:, cols] = x_ref[...].astype(F32) + (dot(a_ref[...], wa_all[...]) + dot(b_ref[...], wb_all[...]))

    @pl.when(step == out_steps - 1)
    def _():
        u_ref[:half, :] = normed(mid_ref[other, :], gain_ref[...])
        u_ref[half:, :] = normed(mid_ref[own, :], gain_ref[...])
        acc_ref[...] = jnp.zeros_like(acc_ref)

    @pl.when(step >= out_steps)
    def _():
        u = u_ref[...]
        gate = dot(u, wg_ref[...])
        hidden = (gate * jax.nn.sigmoid(gate) * dot(u, wu_ref[...])).astype(BF16)
        acc_ref[...] += dot(hidden, wd_ref[...])

    @pl.when(step == pl.num_programs(0) - 1)
    def _():
        send_ref[...] = acc_ref[:half, :]
        keep_ref[...] = mid_ref[own, :] + acc_ref[half:, :]


def chunk_layer(meta, x, chunk, attn_mine, attn_peer, wo_mine, wo_pieces, gain, w_gate, w_up, w_down):
    rows, depth = attn_mine.shape
    dim, ff = w_gate.shape
    block = 512
    out_steps, mlp_steps = dim // block, ff // FF_BLOCK
    heads = 4
    resident = lambda a, b: pl.BlockSpec((a, b), lambda i, m: (0, 0))
    early = lambda i: jnp.minimum(i, out_steps - 1)
    late = lambda i: jnp.maximum(i - out_steps, 0)
    mine_specs = [pl.BlockSpec((depth // heads, block), lambda i, m, p=p: (p ^ m[0], early(i))) for p in range(heads)]
    peer_specs = [pl.BlockSpec((w.shape[0], block), lambda i, m: (0, early(i))) for w in wo_pieces]
    return pl.pallas_call(
        functools.partial(chunk_kernel, heads, len(wo_pieces), out_steps), name="chunk_layer",
        grid_spec=pltpu.PrefetchScalarGridSpec(
            num_scalar_prefetch=1, grid=(out_steps + mlp_steps,),
            in_specs=[pl.BlockSpec((rows, block), lambda i, m: (chunk, early(i))), resident(rows, depth), resident(rows, depth),
                      resident(1, dim)] + mine_specs + peer_specs
                     + [pl.BlockSpec((dim, FF_BLOCK), lambda i, m: (0, late(i))), pl.BlockSpec((dim, FF_BLOCK), lambda i, m: (0, late(i))),
                        pl.BlockSpec((FF_BLOCK, dim), lambda i, m: (late(i), 0))],
            out_specs=[resident(rows // 2, dim)] * 2,
            scratch_shapes=[pltpu.VMEM((rows, dim), F32), pltpu.VMEM((rows, dim), BF16), pltpu.VMEM((rows, dim), F32),
                            pltpu.VMEM((depth, block), BF16), pltpu.VMEM((depth, block), BF16)]),
        out_shape=[jax.ShapeDtypeStruct((rows // 2, dim), F32)] * 2,
        compiler_params=params(("arbitrary",), 60),
        cost_estimate=pl.CostEstimate(flops=4 * rows * depth * dim + 6 * rows * dim * ff, bytes_accessed=6 * dim * ff, transcendentals=0),
    )(meta, x, attn_mine, attn_peer, gain, *([wo_mine] * heads), *wo_pieces, w_gate, w_up, w_down)


def unwritten(shape, dtype):
    return pl.pallas_call(lambda out_ref: None, name="unwritten", out_shape=jax.ShapeDtypeStruct(shape, dtype),
                          out_specs=pl.BlockSpec(memory_space=pl.ANY))()


def solution(mesh):
    sp_size = mesh.shape["sp"]
    row_spec = P(("rep", "sp"), None)
    tok_spec = P(("rep", "sp"))
    full_spec = P(None)
    col_spec = P(None, "tp")
    wrow_spec = P("tp", None)
    cache_spec = P("rep", ("tp", "sp"), None)
    tp_swap = [(0, 1), (1, 0)]
    core_swap = [(i, i ^ 1) for i in range(sp_size)]
    chip_swap = [(i, i ^ 2) for i in range(sp_size)]

    def layer(x_in, positions, segments, gain_attn, w_q, w_k, w_v, w_o, gain_mlp, w_gate, w_up, w_down):
        rows_local, dim = x_in.shape
        tp_idx, sp_idx = lax.axis_index("tp"), lax.axis_index("sp")
        odd, high = (sp_idx & 1) == 1, (sp_idx & 2) == 2

        depth = w_o.shape[0]
        quarter = depth // sp_size
        half_q = quarter // 2
        wo_own = lax.ppermute(lax.dynamic_slice(w_o, (sp_idx * quarter, 0), (quarter, dim)), "tp", tp_swap)
        wo_far = lax.ppermute(lax.dynamic_slice(w_o, ((sp_idx ^ 2) * quarter, 0), (half_q, dim)), "tp", tp_swap)

        zeros = jnp.sum((segments == 0).astype(jnp.int32)).reshape(1)
        zeros = zeros + lax.ppermute(zeros, "sp", core_swap)
        cut = (zeros + lax.ppermute(zeros, "sp", chip_swap))[0]
        meta = jnp.stack([sp_idx, cut, tp_idx, 1 - tp_idx]).astype(jnp.int32)

        cos_t, sin_t = rope_tables(positions)
        gain_a, gain_m = gain_attn.reshape(1, dim), gain_mlp.reshape(1, dim)
        u, kv_own = project_kv(x_in, gain_a, w_k, w_v, cos_t, sin_t)
        kv_chip = lax.ppermute(kv_own, "sp", chip_swap)
        kv_core = lax.ppermute(kv_own, "sp", core_swap)
        kv_diag = lax.ppermute(kv_chip, "sp", core_swap)
        kv_parts = (kv_own, kv_core, kv_chip, kv_diag)
        q_rot = project_q(u, w_q, cos_t, sin_t)

        wo_near = lax.ppermute(wo_own[half_q:], "sp", chip_swap)
        wo_core = lax.ppermute(wo_own, "sp", core_swap)
        wo_dfar = lax.ppermute(wo_far, "sp", core_swap)
        wo_dnear = lax.ppermute(wo_near, "sp", core_swap)
        wo_pieces = (wo_own, wo_core, wo_far, wo_near, wo_dfar, wo_dnear)

        def ordered(own, core, chip, diag):
            near = jnp.concatenate([jnp.where(odd, core, own), jnp.where(odd, own, core)], axis=0)
            far = jnp.concatenate([jnp.where(odd, diag, chip), jnp.where(odd, chip, diag)], axis=0)
            return jnp.concatenate([jnp.where(high, far, near), jnp.where(high, near, far)], axis=0)

        def cache(offset):
            cols = [lax.dynamic_slice(part, (0, offset + sp_idx * HEAD_DIM), (rows_local, HEAD_DIM)) for part in kv_parts]
            return ordered(*cols).reshape(sp_size * rows_local, 1, HEAD_DIM)

        chunk_rows = rows_local // CHUNKS
        half = chunk_rows // 2
        attn_flops = 4 * chunk_rows * sp_size * rows_local * w_q.shape[1] // 4
        split = CHUNKS // 2
        partial_sums = attention(meta, q_rot, kv_parts[:2], 0, split * chunk_rows, 512, attn_flops, False)
        attn_mine, attn_peer = [], []
        for c in range(CHUNKS):
            if c < split:
                rest = (kv_parts[2:], c * chunk_rows, chunk_rows, 1024, attn_flops, True, partial_sums)
            else:
                rest = (kv_parts, c * chunk_rows, chunk_rows, 1024, attn_flops)
            attn_mine.append(attention(meta, q_rot, *rest))
            attn_peer.append(lax.ppermute(attn_mine[c], "tp", tp_swap))
        k_cache, v_cache = cache(0), cache(w_k.shape[1])
        y_out = unwritten((rows_local, dim), BF16)

        kept, sent = [], []
        for c in range(CHUNKS):
            p_peer, p_own = chunk_layer(meta, x_in, c, attn_mine[c], attn_peer[c], w_o, wo_pieces, gain_m,
                                   w_gate, w_up, w_down)
            sent.append(lax.ppermute(p_peer, "tp", tp_swap))
            kept.append(p_own)
        for c in range(CHUNKS):
            y_own = lax.optimization_barrier((kept[c] + sent[c]).astype(BF16))
            y_peer = lax.ppermute(y_own, "tp", tp_swap)
            y_out = lax.dynamic_update_slice(y_out, y_own, (c * chunk_rows + tp_idx * half, 0))
            y_out = lax.dynamic_update_slice(y_out, y_peer, (c * chunk_rows + (1 - tp_idx) * half, 0))
        return y_out, k_cache, v_cache


    return jax.shard_map(layer, mesh=mesh,
                         in_specs=(row_spec, tok_spec, tok_spec, full_spec, col_spec, col_spec, col_spec, wrow_spec,
                                   full_spec, col_spec, col_spec, wrow_spec),
                         out_specs=(row_spec, cache_spec, cache_spec), check_vma=False)
```

```python
import functools
import jax
import jax.numpy as jnp
from jax import lax
from jax.experimental import pallas as pl
from jax.experimental.pallas import tpu as pltpu
from jax.sharding import PartitionSpec as P


HEAD_DIM = 128
HALF = HEAD_DIM // 2
ROPE_BASE = 500000.0
NORM_EPS = 1e-5
LOG2E = 1.4426950408889634
BF16 = jnp.bfloat16
F32 = jnp.float32

CHUNKS = 4
Q_BLOCK = 256
FF_BLOCK = 512
MASKED = -1e30


def params(semantics, mib):
    return pltpu.CompilerParams(dimension_semantics=semantics, vmem_limit_bytes=mib << 20)


def dot(a, b):
    return jnp.dot(a, b, preferred_element_type=F32)


def normed(x, gain):
    mean_sq = jnp.mean(x * x, axis=-1, keepdims=True)
    return (x * lax.rsqrt(mean_sq + NORM_EPS) * gain).astype(BF16)


def rope_tables(positions):
    inv_freq = jnp.power(jnp.float32(ROPE_BASE), -jnp.arange(HALF, dtype=F32) * (2.0 / HEAD_DIM))
    angles = positions.astype(F32)[:, None] * jnp.concatenate([inv_freq, inv_freq])
    sign = jnp.where(jnp.arange(HEAD_DIM) < HALF, -1.0, 1.0).astype(F32)
    return jnp.cos(angles), jnp.sin(angles) * sign


def store_rotated(out_ref, rows, t_f32, cos_t, sin_t):
    for head in range(t_f32.shape[1] // HEAD_DIM):
        cols = slice(head * HEAD_DIM, (head + 1) * HEAD_DIM)
        t_head = t_f32[:, cols]
        out_ref[rows, cols] = (t_head * cos_t + pltpu.roll(t_head, HALF, 1) * sin_t).astype(BF16)


def kv_kernel(x_ref, gain_ref, wk_ref, wv_ref, cos_ref, sin_ref, u_ref, kv_ref):
    u = normed(x_ref[...].astype(F32), gain_ref[...])
    u_ref[...] = u
    width = wk_ref.shape[1]
    store_rotated(kv_ref, slice(None), dot(u, wk_ref[...]), cos_ref[...], sin_ref[...])
    kv_ref[:, width:] = dot(u, wv_ref[...]).astype(BF16)


def project_kv(x, gain, w_k, w_v, cos_t, sin_t):
    rows, dim = x.shape
    width = w_k.shape[1]
    block = 256
    whole = lambda a, b: pl.BlockSpec((a, b), lambda i: (0, 0))
    banded = lambda b: pl.BlockSpec((block, b), lambda i: (i, 0))
    return pl.pallas_call(
        kv_kernel, grid=(rows // block,), name="project_kv",
        in_specs=[banded(dim), whole(1, dim), whole(dim, width), whole(dim, width), banded(HEAD_DIM), banded(HEAD_DIM)],
        out_specs=[banded(dim), banded(2 * width)],
        out_shape=[jax.ShapeDtypeStruct((rows, dim), BF16), jax.ShapeDtypeStruct((rows, 2 * width), BF16)],
        compiler_params=params(("arbitrary",), 48),
        cost_estimate=pl.CostEstimate(flops=4 * rows * dim * width, bytes_accessed=4 * dim * (rows + width), transcendentals=0),
    )(x, gain, w_k, w_v, cos_t, sin_t)


def q_kernel(u_ref, w_ref, cos_ref, sin_ref, q_ref):
    block = 512

    @pl.loop(0, u_ref.shape[0] // block)
    def _(i):
        rows = pl.ds(pl.multiple_of(i * block, block), block)
        store_rotated(q_ref, rows, dot(u_ref[rows, :], w_ref[...]), cos_ref[rows, :], sin_ref[rows, :])


def project_q(u, w_q, cos_t, sin_t):
    rows, dim = u.shape
    width = w_q.shape[1]
    block = 512
    return pl.pallas_call(
        q_kernel, grid=(width // block,), name="project_q",
        in_specs=[pl.BlockSpec((rows, dim), lambda i: (0, 0)), pl.BlockSpec((dim, block), lambda i: (0, i)),
                  pl.BlockSpec((rows, HEAD_DIM), lambda i: (0, 0)), pl.BlockSpec((rows, HEAD_DIM), lambda i: (0, 0))],
        out_specs=pl.BlockSpec((rows, block), lambda i: (0, i)),
        out_shape=jax.ShapeDtypeStruct((rows, width), BF16),
        compiler_params=params(("arbitrary",), 48),
        cost_estimate=pl.CostEstimate(flops=2 * rows * dim * width, bytes_accessed=2 * dim * (rows + width), transcendentals=0),
    )(u, w_q, cos_t, sin_t)


def attn_kernel(group, row_base, parts, k_block, load, finish, meta_ref, q_ref, *refs):
    k_refs, v_refs, refs = refs[:parts], refs[parts:2 * parts], refs[2 * parts:]
    if load:
        acc_in, m_in, l_in = refs[:3]
    if finish:
        o_ref = refs[-7]
    else:
        acc_out, m_out, l_out = refs[:3]
    k_all, v_all, q_t, m_ref, l_ref, acc_ref = refs[-6:]
    shard, cut = meta_ref[0], meta_ref[1]
    block = q_ref.shape[0]
    keys = k_refs[0].shape[0]
    scale = (HEAD_DIM ** -0.5) * LOG2E
    chip_base = (shard // 2) * (2 * keys)
    base = 0 if finish else chip_base

    @pl.when(pl.program_id(1) == 0)
    def _():
        for idx in range(parts):
            rows = pl.ds(pl.multiple_of(((shard ^ idx) & (parts - 1)) * keys, keys), keys)
            k_all[rows, :] = k_refs[idx][...]
            v_all[:, rows] = v_refs[idx][...].T

    first = shard * keys + row_base + pl.program_id(1) * block
    last = first + block - 1
    for head in range(group):
        q_t[head] = q_ref[:, head * HEAD_DIM:(head + 1) * HEAD_DIM].T
    if load:
        m_ref[...], l_ref[...], acc_ref[...] = m_in[...], l_in[...], acc_in[...]
    else:
        m_ref[...] = jnp.full_like(m_ref, MASKED)
        l_ref[...] = jnp.zeros_like(l_ref)
        acc_ref[...] = jnp.zeros_like(acc_ref)

    def step(masked, kb, carry):
        start = kb * k_block
        rows = pl.ds(pl.multiple_of(start - base, k_block), k_block)
        k_blk = k_all[rows, :]
        v_blk = v_all[:, rows]
        scores = [dot(k_blk, q_t[head]) for head in range(group)]
        m_old = [m_ref[head] for head in range(group)]
        l_old = [l_ref[head] for head in range(group)]
        if masked:
            k_idx = start + lax.broadcasted_iota(jnp.int32, (k_block, block), 0)
            r_idx = first + lax.broadcasted_iota(jnp.int32, (k_block, block), 1)
            allowed = (k_idx <= r_idx) & ((k_idx >= cut) | (r_idx < cut))
            scores = [jnp.where(allowed, s, MASKED) for s in scores]
        news = []
        for head in range(group):
            m_new = jnp.maximum(m_old[head], jnp.max(scores[head], axis=0, keepdims=True) * scale)
            p = jnp.exp2(scores[head] * scale - m_new)
            alpha = jnp.exp2(m_old[head] - m_new)
            total = alpha * l_old[head] + jnp.sum(p, axis=0, keepdims=True)
            news.append((m_new, total, alpha, dot(v_blk, p.astype(BF16))))
        for head in range(group):
            m_ref[head], l_ref[head] = news[head][:2]
            acc_ref[head] = news[head][2] * acc_ref[head] + news[head][3]
        return carry

    seg_low = jnp.where(first >= cut, cut, 0)
    seg_high = jnp.where(last >= cut, cut, 0)
    low = jnp.maximum(seg_low, base) // k_block
    high = chip_base // k_block if load else last // k_block + 1
    clear = (seg_high + k_block - 1) // k_block
    edge_a = jnp.maximum(low, jnp.minimum(clear, high))
    edge_b = jnp.maximum(edge_a, jnp.minimum((first + 1) // k_block, high))
    head_count = edge_a - low
    lax.fori_loop(edge_a, edge_b, functools.partial(step, False), 0)
    lax.fori_loop(0, head_count + jnp.maximum(high - edge_b, 0),
                  lambda i, carry: step(True, jnp.where(i < head_count, low + i, edge_b + i - head_count), carry), 0)
    if finish:
        for head in range(group):
            o_ref[:, head * HEAD_DIM:(head + 1) * HEAD_DIM] = (acc_ref[head] / l_ref[head]).T.astype(BF16)
    else:
        acc_out[...], m_out[...], l_out[...] = acc_ref[...], m_ref[...], l_ref[...]


def attention(meta, q_rot, kv_parts, row_base, rows, k_block, flops, finish=True, partial_sums=None):
    kv_rows, kv_width = kv_parts[0].shape
    kv_heads = kv_width // (2 * HEAD_DIM)
    group = q_rot.shape[1] // HEAD_DIM // kv_heads
    width = group * HEAD_DIM
    base = row_base // Q_BLOCK
    parts, load = len(kv_parts), partial_sums is not None
    k_spec = pl.BlockSpec((kv_rows, HEAD_DIM), lambda h, i, m: (0, h))
    v_spec = pl.BlockSpec((kv_rows, HEAD_DIM), lambda h, i, m: (0, kv_heads + h))
    sums_specs = [pl.BlockSpec((group, depth, Q_BLOCK), lambda h, i, m: (h, 0, base + i)) for depth in (HEAD_DIM, 1, 1)]
    sums_shapes = [jax.ShapeDtypeStruct((kv_heads * group, depth, rows), F32) for depth in (HEAD_DIM, 1, 1)]
    return pl.pallas_call(
        functools.partial(attn_kernel, group, row_base, parts, k_block, load, finish), name="attention",
        grid_spec=pltpu.PrefetchScalarGridSpec(
            num_scalar_prefetch=1, grid=(kv_heads, rows // Q_BLOCK),
            in_specs=[pl.BlockSpec((Q_BLOCK, width), lambda h, i, m: (base + i, h))] + [k_spec] * parts + [v_spec] * parts
                     + (sums_specs if load else []),
            out_specs=pl.BlockSpec((Q_BLOCK, width), lambda h, i, m: (i, h ^ m[0])) if finish else sums_specs,
            scratch_shapes=[pltpu.VMEM((parts * kv_rows, HEAD_DIM), BF16), pltpu.VMEM((HEAD_DIM, parts * kv_rows), BF16),
                            pltpu.VMEM((group, HEAD_DIM, Q_BLOCK), BF16), pltpu.VMEM((group, 1, Q_BLOCK), F32),
                            pltpu.VMEM((group, 1, Q_BLOCK), F32), pltpu.VMEM((group, HEAD_DIM, Q_BLOCK), F32)]),
        out_shape=jax.ShapeDtypeStruct((rows, kv_heads * width), BF16) if finish else sums_shapes,
        compiler_params=params(("arbitrary", "arbitrary"), 48),
        cost_estimate=pl.CostEstimate(flops=flops, bytes_accessed=16 << 20, transcendentals=0),
    )(meta, q_rot, *kv_parts, *kv_parts, *(partial_sums or ()))


def chunk_kernel(mine, peer, out_steps, meta_ref, x_ref, a_ref, b_ref, gain_ref, *refs):
    wa_refs, wb_refs = refs[:mine], refs[mine:mine + peer]
    wg_ref, wu_ref, wd_ref, send_ref, keep_ref, mid_ref, u_ref, acc_ref, wa_all, wb_all = refs[mine + peer:]
    step = pl.program_id(0)
    half = send_ref.shape[0]
    own = pl.ds(pl.multiple_of(meta_ref[2] * half, half), half)
    other = pl.ds(pl.multiple_of(meta_ref[3] * half, half), half)

    @pl.when(step < out_steps)
    def _():
        width = wa_all.shape[1]
        for pieces, whole in ((wa_refs, wa_all), (wb_refs, wb_all)):
            top = 0
            for piece in pieces:
                whole[top:top + piece.shape[0], :] = piece[...]
                top += piece.shape[0]
        cols = pl.ds(pl.multiple_of(step * width, width), width)
        mid_ref[:, cols] = x_ref[...].astype(F32) + (dot(a_ref[...], wa_all[...]) + dot(b_ref[...], wb_all[...]))

    @pl.when(step == out_steps - 1)
    def _():
        u_ref[:half, :] = normed(mid_ref[other, :], gain_ref[...])
        u_ref[half:, :] = normed(mid_ref[own, :], gain_ref[...])
        acc_ref[...] = jnp.zeros_like(acc_ref)

    @pl.when(step >= out_steps)
    def _():
        u = u_ref[...]
        gate = dot(u, wg_ref[...])
        hidden = (gate * jax.nn.sigmoid(gate) * dot(u, wu_ref[...])).astype(BF16)
        acc_ref[...] += dot(hidden, wd_ref[...])

    @pl.when(step == pl.num_programs(0) - 1)
    def _():
        send_ref[...] = acc_ref[:half, :]
        keep_ref[...] = mid_ref[own, :] + acc_ref[half:, :]


def chunk_layer(meta, x, chunk, attn_mine, attn_peer, wo_mine, wo_pieces, gain, w_gate, w_up, w_down):
    rows, depth = attn_mine.shape
    dim, ff = w_gate.shape
    block = 512
    out_steps, mlp_steps = dim // block, ff // FF_BLOCK
    heads = 4
    resident = lambda a, b: pl.BlockSpec((a, b), lambda i, m: (0, 0))
    early = lambda i: jnp.minimum(i, out_steps - 1)
    late = lambda i: jnp.maximum(i - out_steps, 0)
    mine_specs = [pl.BlockSpec((depth // heads, block), lambda i, m, p=p: (p ^ m[0], early(i))) for p in range(heads)]
    peer_specs = [pl.BlockSpec((w.shape[0], block), lambda i, m: (0, early(i))) for w in wo_pieces]
    return pl.pallas_call(
        functools.partial(chunk_kernel, heads, len(wo_pieces), out_steps), name="chunk_layer",
        grid_spec=pltpu.PrefetchScalarGridSpec(
            num_scalar_prefetch=1, grid=(out_steps + mlp_steps,),
            in_specs=[pl.BlockSpec((rows, block), lambda i, m: (chunk, early(i))), resident(rows, depth), resident(rows, depth),
                      resident(1, dim)] + mine_specs + peer_specs
                     + [pl.BlockSpec((dim, FF_BLOCK), lambda i, m: (0, late(i))), pl.BlockSpec((dim, FF_BLOCK), lambda i, m: (0, late(i))),
                        pl.BlockSpec((FF_BLOCK, dim), lambda i, m: (late(i), 0))],
            out_specs=[resident(rows // 2, dim)] * 2,
            scratch_shapes=[pltpu.VMEM((rows, dim), F32), pltpu.VMEM((rows, dim), BF16), pltpu.VMEM((rows, dim), F32),
                            pltpu.VMEM((depth, block), BF16), pltpu.VMEM((depth, block), BF16)]),
        out_shape=[jax.ShapeDtypeStruct((rows // 2, dim), F32)] * 2,
        compiler_params=params(("arbitrary",), 60),
        cost_estimate=pl.CostEstimate(flops=4 * rows * depth * dim + 6 * rows * dim * ff, bytes_accessed=6 * dim * ff, transcendentals=0),
    )(meta, x, attn_mine, attn_peer, gain, *([wo_mine] * heads), *wo_pieces, w_gate, w_up, w_down)


def unwritten(shape, dtype):
    return pl.pallas_call(lambda out_ref: None, name="unwritten", out_shape=jax.ShapeDtypeStruct(shape, dtype),
                          out_specs=pl.BlockSpec(memory_space=pltpu.HBM))()


def finish_kernel(meta_ref, kept_ref, sent_ref, y_in, own_ref, y_ref):
    y_own = (kept_ref[...] + sent_ref[...]).astype(BF16)
    own_ref[...] = y_own
    y_ref[...] = y_own


def finish_rows(meta, chunk, kept, sent, y_out):
    rows, dim = kept.shape
    whole = pl.BlockSpec((rows, dim), lambda i, m: (0, 0))
    return pl.pallas_call(
        finish_kernel, name="finish_rows",
        grid_spec=pltpu.PrefetchScalarGridSpec(
            num_scalar_prefetch=1, grid=(1,), in_specs=[whole, whole, pl.BlockSpec(memory_space=pltpu.HBM)],
            out_specs=[whole, pl.BlockSpec((rows, dim), lambda i, m: (2 * chunk + m[2], 0))]),
        out_shape=[jax.ShapeDtypeStruct((rows, dim), BF16), jax.ShapeDtypeStruct(y_out.shape, BF16)],
        input_output_aliases={3: 1},
        compiler_params=params(("arbitrary",), 32),
        cost_estimate=pl.CostEstimate(flops=rows * dim, bytes_accessed=12 * rows * dim, transcendentals=0),
    )(meta, kept, sent, y_out)


def place_kernel(meta_ref, piece_ref, y_in, y_ref):
    y_ref[...] = piece_ref[...]


def place_rows(meta, chunk, piece, y_out):
    rows, dim = piece.shape
    return pl.pallas_call(
        place_kernel, name="place_rows",
        grid_spec=pltpu.PrefetchScalarGridSpec(
            num_scalar_prefetch=1, grid=(1,),
            in_specs=[pl.BlockSpec((rows, dim), lambda i, m: (0, 0)), pl.BlockSpec(memory_space=pltpu.HBM)],
            out_specs=pl.BlockSpec((rows, dim), lambda i, m: (2 * chunk + m[3], 0))),
        out_shape=jax.ShapeDtypeStruct(y_out.shape, BF16),
        input_output_aliases={2: 0},
        compiler_params=params(("arbitrary",), 32),
        cost_estimate=pl.CostEstimate(flops=rows * dim, bytes_accessed=4 * rows * dim, transcendentals=0),
    )(meta, piece, y_out)


def solution(mesh):
    sp_size = mesh.shape["sp"]
    row_spec = P(("rep", "sp"), None)
    tok_spec = P(("rep", "sp"))
    full_spec = P(None)
    col_spec = P(None, "tp")
    wrow_spec = P("tp", None)
    cache_spec = P("rep", ("tp", "sp"), None)
    tp_swap = [(0, 1), (1, 0)]
    core_swap = [(i, i ^ 1) for i in range(sp_size)]
    chip_swap = [(i, i ^ 2) for i in range(sp_size)]

    def layer(x_in, positions, segments, gain_attn, w_q, w_k, w_v, w_o, gain_mlp, w_gate, w_up, w_down):
        rows_local, dim = x_in.shape
        tp_idx, sp_idx = lax.axis_index("tp"), lax.axis_index("sp")
        odd, high = (sp_idx & 1) == 1, (sp_idx & 2) == 2

        depth = w_o.shape[0]
        quarter = depth // sp_size
        half_q = quarter // 2

        def wo_rows(index, second):
            return lax.dynamic_slice(w_o, (index * quarter + second * half_q, 0), (half_q, dim))

        wo_a = lax.ppermute(wo_rows(sp_idx, 0), "tp", tp_swap)

        zeros = jnp.sum((segments == 0).astype(jnp.int32)).reshape(1)
        zeros = zeros + lax.ppermute(zeros, "sp", core_swap)
        cut = (zeros + lax.ppermute(zeros, "sp", chip_swap))[0]
        meta = jnp.stack([sp_idx, cut, tp_idx, 1 - tp_idx]).astype(jnp.int32)

        cos_t, sin_t = rope_tables(positions)
        gain_a, gain_m = gain_attn.reshape(1, dim), gain_mlp.reshape(1, dim)
        u, kv_own = project_kv(x_in, gain_a, w_k, w_v, cos_t, sin_t)
        kv_chip = lax.ppermute(kv_own, "sp", chip_swap)
        kv_core = lax.ppermute(kv_own, "sp", core_swap)
        kv_diag = lax.ppermute(kv_chip, "sp", core_swap)
        kv_parts = (kv_own, kv_core, kv_chip, kv_diag)
        q_rot = project_q(u, w_q, cos_t, sin_t)

        wo_b = lax.ppermute(wo_rows(sp_idx, 1), "tp", tp_swap)
        wo_far = lax.ppermute(wo_rows(sp_idx ^ 2, 1), "tp", tp_swap)
        wo_near = lax.ppermute(wo_a, "sp", chip_swap)
        wo_core = [lax.ppermute(piece, "sp", core_swap) for piece in
                   (wo_a, wo_b, wo_near, wo_far)]
        wo_pieces = (wo_a, wo_b, wo_core[0], wo_core[1], wo_near, wo_far, wo_core[2], wo_core[3])

        def ordered(own, core, chip, diag):
            near = jnp.concatenate([jnp.where(odd, core, own), jnp.where(odd, own, core)], axis=0)
            far = jnp.concatenate([jnp.where(odd, diag, chip), jnp.where(odd, chip, diag)], axis=0)
            return jnp.concatenate([jnp.where(high, far, near), jnp.where(high, near, far)], axis=0)

        def cache(offset):
            cols = [lax.dynamic_slice(part, (0, offset + sp_idx * HEAD_DIM), (rows_local, HEAD_DIM)) for part in kv_parts]
            return ordered(*cols).reshape(sp_size * rows_local, 1, HEAD_DIM)

        chunk_rows = rows_local // CHUNKS
        attn_flops = 4 * chunk_rows * sp_size * rows_local * w_q.shape[1] // 4
        split = CHUNKS // 2
        partial_sums = attention(meta, q_rot, kv_parts[:2], 0, split * chunk_rows, 512, attn_flops, False)
        attn_mine, attn_peer = [], []
        for c in range(CHUNKS):
            if c < split:
                rest = (kv_parts[2:], c * chunk_rows, chunk_rows, 1024, attn_flops, True, partial_sums)
            else:
                rest = (kv_parts, c * chunk_rows, chunk_rows, 1024, attn_flops)
            attn_mine.append(attention(meta, q_rot, *rest))
            attn_peer.append(lax.ppermute(attn_mine[c], "tp", tp_swap))
        k_cache, v_cache = cache(0), cache(w_k.shape[1])
        y_out = unwritten((rows_local, dim), BF16)

        kept, sent = [], []
        for c in range(CHUNKS):
            p_peer, p_own = chunk_layer(meta, x_in, c, attn_mine[c], attn_peer[c], w_o, wo_pieces, gain_m,
                                   w_gate, w_up, w_down)
            sent.append(lax.ppermute(p_peer, "tp", tp_swap))
            kept.append(p_own)
        y_peer = []
        for c in range(CHUNKS):
            y_own, y_out = finish_rows(meta, c, kept[c], sent[c], y_out)
            y_peer.append(lax.ppermute(y_own, "tp", tp_swap))
        for c in range(CHUNKS):
            y_out = place_rows(meta, c, y_peer[c], y_out)
        return y_out, k_cache, v_cache


    return jax.shard_map(layer, mesh=mesh,
                         in_specs=(row_spec, tok_spec, tok_spec, full_spec, col_spec, col_spec, col_spec, wrow_spec,
                                   full_spec, col_spec, col_spec, wrow_spec),
                         out_specs=(row_spec, cache_spec, cache_spec), check_vma=False)
```

```python
import functools
import jax
import jax.numpy as jnp
from jax import lax
from jax.experimental import pallas as pl
from jax.experimental.pallas import tpu as pltpu
from jax.sharding import PartitionSpec as P


HEAD_DIM = 128
HALF = HEAD_DIM // 2
ROPE_BASE = 500000.0
NORM_EPS = 1e-5
LOG2E = 1.4426950408889634
BF16 = jnp.bfloat16
F32 = jnp.float32

CHUNKS = 4
Q_BLOCK = 256
FF_BLOCK = 512
HEAD_GROUPS = 4
MASKED = -1e30


def params(semantics, mib):
    return pltpu.CompilerParams(dimension_semantics=semantics, vmem_limit_bytes=mib << 20)


def dot(a, b):
    return jnp.dot(a, b, preferred_element_type=F32)


def normed(x, gain):
    mean_sq = jnp.mean(x * x, axis=-1, keepdims=True)
    return (x * lax.rsqrt(mean_sq + NORM_EPS) * gain).astype(BF16)


def rope_tables(positions):
    inv_freq = jnp.power(jnp.float32(ROPE_BASE), -jnp.arange(HALF, dtype=F32) * (2.0 / HEAD_DIM))
    angles = positions.astype(F32)[:, None] * jnp.concatenate([inv_freq, inv_freq])
    sign = jnp.where(jnp.arange(HEAD_DIM) < HALF, -1.0, 1.0).astype(F32)
    return jnp.cos(angles), jnp.sin(angles) * sign


def store_rotated(out_ref, rows, t_f32, cos_t, sin_t):
    for head in range(t_f32.shape[1] // HEAD_DIM):
        cols = slice(head * HEAD_DIM, (head + 1) * HEAD_DIM)
        t_head = t_f32[:, cols]
        out_ref[rows, cols] = (t_head * cos_t + pltpu.roll(t_head, HALF, 1) * sin_t).astype(BF16)


def kv_kernel(x_ref, gain_ref, wk_ref, wv_ref, cos_ref, sin_ref, u_ref, kv_ref):
    u = normed(x_ref[...].astype(F32), gain_ref[...])
    u_ref[...] = u
    width = wk_ref.shape[1]
    store_rotated(kv_ref, slice(None), dot(u, wk_ref[...]), cos_ref[...], sin_ref[...])
    kv_ref[:, width:] = dot(u, wv_ref[...]).astype(BF16)


def project_kv(x, gain, w_k, w_v, cos_t, sin_t):
    rows, dim = x.shape
    width = w_k.shape[1]
    block = 256
    whole = lambda a, b: pl.BlockSpec((a, b), lambda i: (0, 0))
    banded = lambda b: pl.BlockSpec((block, b), lambda i: (i, 0))
    return pl.pallas_call(
        kv_kernel, grid=(rows // block,), name="project_kv",
        in_specs=[banded(dim), whole(1, dim), whole(dim, width), whole(dim, width), banded(HEAD_DIM), banded(HEAD_DIM)],
        out_specs=[banded(dim), banded(2 * width)],
        out_shape=[jax.ShapeDtypeStruct((rows, dim), BF16), jax.ShapeDtypeStruct((rows, 2 * width), BF16)],
        compiler_params=params(("arbitrary",), 48),
        cost_estimate=pl.CostEstimate(flops=4 * rows * dim * width, bytes_accessed=4 * dim * (rows + width), transcendentals=0),
    )(x, gain, w_k, w_v, cos_t, sin_t)


def q_kernel(u_ref, w_ref, cos_ref, sin_ref, q_ref):
    block = 512

    @pl.loop(0, u_ref.shape[0] // block)
    def _(i):
        rows = pl.ds(pl.multiple_of(i * block, block), block)
        store_rotated(q_ref, rows, dot(u_ref[rows, :], w_ref[...]), cos_ref[rows, :], sin_ref[rows, :])


def project_q(u, w_q, cos_t, sin_t):
    rows, dim = u.shape
    width = w_q.shape[1]
    block = 512
    return pl.pallas_call(
        q_kernel, grid=(width // block,), name="project_q",
        in_specs=[pl.BlockSpec((rows, dim), lambda i: (0, 0)), pl.BlockSpec((dim, block), lambda i: (0, i)),
                  pl.BlockSpec((rows, HEAD_DIM), lambda i: (0, 0)), pl.BlockSpec((rows, HEAD_DIM), lambda i: (0, 0))],
        out_specs=pl.BlockSpec((rows, block), lambda i: (0, i)),
        out_shape=jax.ShapeDtypeStruct((rows, width), BF16),
        compiler_params=params(("arbitrary",), 48),
        cost_estimate=pl.CostEstimate(flops=2 * rows * dim * width, bytes_accessed=2 * dim * (rows + width), transcendentals=0),
    )(u, w_q, cos_t, sin_t)


def attn_kernel(group, row_base, parts, k_block, load, finish, meta_ref, q_ref, *refs):
    k_refs, v_refs, refs = refs[:parts], refs[parts:2 * parts], refs[2 * parts:]
    if load:
        acc_in, m_in, l_in = refs[:3]
    if finish:
        o_ref = refs[-7]
    else:
        acc_out, m_out, l_out = refs[:3]
    k_all, v_all, q_t, m_ref, l_ref, acc_ref = refs[-6:]
    shard, cut = meta_ref[0], meta_ref[1]
    block = q_ref.shape[0]
    keys = k_refs[0].shape[0]
    scale = (HEAD_DIM ** -0.5) * LOG2E
    chip_base = (shard // 2) * (2 * keys)
    base = 0 if finish else chip_base

    @pl.when(pl.program_id(1) == 0)
    def _():
        for idx in range(parts):
            rows = pl.ds(pl.multiple_of(((shard ^ idx) & (parts - 1)) * keys, keys), keys)
            k_all[rows, :] = k_refs[idx][...]
            v_all[:, rows] = v_refs[idx][...].T

    first = shard * keys + row_base + pl.program_id(1) * block
    last = first + block - 1
    for head in range(group):
        q_t[head] = q_ref[:, head * HEAD_DIM:(head + 1) * HEAD_DIM].T
    if load:
        m_ref[...], l_ref[...], acc_ref[...] = m_in[...], l_in[...], acc_in[...]
    else:
        m_ref[...] = jnp.full_like(m_ref, MASKED)
        l_ref[...] = jnp.zeros_like(l_ref)
        acc_ref[...] = jnp.zeros_like(acc_ref)

    def step(masked, kb, carry):
        start = kb * k_block
        rows = pl.ds(pl.multiple_of(start - base, k_block), k_block)
        k_blk = k_all[rows, :]
        v_blk = v_all[:, rows]
        scores = [dot(k_blk, q_t[head]) for head in range(group)]
        m_old = [m_ref[head] for head in range(group)]
        l_old = [l_ref[head] for head in range(group)]
        if masked:
            k_idx = start + lax.broadcasted_iota(jnp.int32, (k_block, block), 0)
            r_idx = first + lax.broadcasted_iota(jnp.int32, (k_block, block), 1)
            allowed = (k_idx <= r_idx) & ((k_idx >= cut) | (r_idx < cut))
            scores = [jnp.where(allowed, s, MASKED) for s in scores]
        news = []
        for head in range(group):
            m_new = jnp.maximum(m_old[head], jnp.max(scores[head], axis=0, keepdims=True) * scale)
            p = jnp.exp2(scores[head] * scale - m_new)
            alpha = jnp.exp2(m_old[head] - m_new)
            total = alpha * l_old[head] + jnp.sum(p, axis=0, keepdims=True)
            news.append((m_new, total, alpha, dot(v_blk, p.astype(BF16))))
        for head in range(group):
            m_ref[head], l_ref[head] = news[head][:2]
            acc_ref[head] = news[head][2] * acc_ref[head] + news[head][3]
        return carry

    seg_low = jnp.where(first >= cut, cut, 0)
    seg_high = jnp.where(last >= cut, cut, 0)
    low = jnp.maximum(seg_low, base) // k_block
    high = chip_base // k_block if load else last // k_block + 1
    clear = (seg_high + k_block - 1) // k_block
    edge_a = jnp.maximum(low, jnp.minimum(clear, high))
    edge_b = jnp.maximum(edge_a, jnp.minimum((first + 1) // k_block, high))
    head_count = edge_a - low
    lax.fori_loop(edge_a, edge_b, functools.partial(step, False), 0)
    lax.fori_loop(0, head_count + jnp.maximum(high - edge_b, 0),
                  lambda i, carry: step(True, jnp.where(i < head_count, low + i, edge_b + i - head_count), carry), 0)
    if finish:
        for head in range(group):
            o_ref[:, head * HEAD_DIM:(head + 1) * HEAD_DIM] = (acc_ref[head] / l_ref[head]).T.astype(BF16)
    else:
        acc_out[...], m_out[...], l_out[...] = acc_ref[...], m_ref[...], l_ref[...]


def attention(meta, q_rot, kv_parts, row_base, rows, k_block, flops, finish=True, partial_sums=None):
    kv_rows, kv_width = kv_parts[0].shape
    kv_heads = kv_width // (2 * HEAD_DIM)
    group = q_rot.shape[1] // HEAD_DIM // kv_heads
    width = group * HEAD_DIM
    base = row_base // Q_BLOCK
    parts, load = len(kv_parts), partial_sums is not None
    k_spec = pl.BlockSpec((kv_rows, HEAD_DIM), lambda h, i, m: (0, h))
    v_spec = pl.BlockSpec((kv_rows, HEAD_DIM), lambda h, i, m: (0, kv_heads + h))
    sums_specs = [pl.BlockSpec((group, depth, Q_BLOCK), lambda h, i, m: (h, 0, base + i)) for depth in (HEAD_DIM, 1, 1)]
    sums_shapes = [jax.ShapeDtypeStruct((kv_heads * group, depth, rows), F32) for depth in (HEAD_DIM, 1, 1)]
    return pl.pallas_call(
        functools.partial(attn_kernel, group, row_base, parts, k_block, load, finish), name="attention",
        grid_spec=pltpu.PrefetchScalarGridSpec(
            num_scalar_prefetch=1, grid=(kv_heads, rows // Q_BLOCK),
            in_specs=[pl.BlockSpec((Q_BLOCK, width), lambda h, i, m: (base + i, h))] + [k_spec] * parts + [v_spec] * parts
                     + (sums_specs if load else []),
            out_specs=pl.BlockSpec((Q_BLOCK, width), lambda h, i, m: (i, h ^ m[0])) if finish else sums_specs,
            scratch_shapes=[pltpu.VMEM((parts * kv_rows, HEAD_DIM), BF16), pltpu.VMEM((HEAD_DIM, parts * kv_rows), BF16),
                            pltpu.VMEM((group, HEAD_DIM, Q_BLOCK), BF16), pltpu.VMEM((group, 1, Q_BLOCK), F32),
                            pltpu.VMEM((group, 1, Q_BLOCK), F32), pltpu.VMEM((group, HEAD_DIM, Q_BLOCK), F32)]),
        out_shape=jax.ShapeDtypeStruct((rows, kv_heads * width), BF16) if finish else sums_shapes,
        compiler_params=params(("arbitrary", "arbitrary"), 48),
        cost_estimate=pl.CostEstimate(flops=flops, bytes_accessed=16 << 20, transcendentals=0),
    )(meta, q_rot, *kv_parts, *kv_parts, *(partial_sums or ()))


def chunk_kernel(pieces, x_ref, a_ref, b_ref, gain_ref, wo_ref, *refs):
    piece_refs, (wg_ref, wu_ref, wd_ref, send_ref, keep_ref) = refs[:pieces], refs[pieces:pieces + 5]
    mid_ref, u_ref, acc_ref, wa_buf, wb_buf, wg_buf, wu_buf, wd_buf, wo_sem, mlp_sem = refs[pieces + 5:]
    tp_idx, sp_idx = lax.axis_index("tp"), lax.axis_index("sp")
    half = send_ref.shape[0]
    own = pl.ds(pl.multiple_of(tp_idx * half, half), half)
    other = pl.ds(pl.multiple_of((1 - tp_idx) * half, half), half)
    depth, width = wa_buf.shape[1:]
    quarter = depth // HEAD_GROUPS
    out_steps = wo_ref.shape[1] // width
    mlp_steps = wg_ref.shape[1] // FF_BLOCK

    def wo_copies(step, slot):
        cols = pl.ds(pl.multiple_of(step * width, width), width)
        copies, top = [], 0
        for p in range(HEAD_GROUPS):
            rows = pl.ds(pl.multiple_of((p ^ sp_idx) * quarter, quarter), quarter)
            copies.append((wo_ref.at[rows, cols], wa_buf.at[slot, p * quarter:(p + 1) * quarter, :]))
        for piece in piece_refs:
            rows = piece.shape[0]
            copies.append((piece.at[:, cols], wb_buf.at[slot, top:top + rows, :]))
            top += rows
        return [pltpu.make_async_copy(src, dst, wo_sem.at[slot, n]) for n, (src, dst) in enumerate(copies)]

    def mlp_copies(step, slot):
        cols = pl.ds(pl.multiple_of(step * FF_BLOCK, FF_BLOCK), FF_BLOCK)
        copies = ((wg_ref.at[:, cols], wg_buf.at[slot]), (wu_ref.at[:, cols], wu_buf.at[slot]), (wd_ref.at[cols, :], wd_buf.at[slot]))
        return [pltpu.make_async_copy(src, dst, mlp_sem.at[slot, n]) for n, (src, dst) in enumerate(copies)]

    def start(copies):
        for copy in copies:
            copy.start()

    def finish(copies):
        for copy in copies:
            copy.wait()

    start(wo_copies(0, 0))
    start(wo_copies(1, 1))
    acc_ref[...] = jnp.zeros_like(acc_ref)

    def out_step(step, carry):
        slot = step % 2
        finish(wo_copies(step, slot))
        cols = pl.ds(pl.multiple_of(step * width, width), width)
        mid_ref[:, cols] = x_ref[:, cols].astype(F32) + (dot(a_ref[...], wa_buf[slot]) + dot(b_ref[...], wb_buf[slot]))

        @pl.when(step + 2 < out_steps)
        def _():
            start(wo_copies(step + 2, slot))

        @pl.when(step == out_steps - 3)
        def _():
            start(mlp_copies(0, 0))

        return carry

    lax.fori_loop(0, out_steps, out_step, 0)
    start(mlp_copies(1, 1))
    u_ref[:half, :] = normed(mid_ref[other, :], gain_ref[...])
    u_ref[half:, :] = normed(mid_ref[own, :], gain_ref[...])

    def mlp_step(step, carry):
        slot = step % 2
        finish(mlp_copies(step, slot))
        u = u_ref[...]
        gate = dot(u, wg_buf[slot])
        hidden = (gate * jax.nn.sigmoid(gate) * dot(u, wu_buf[slot])).astype(BF16)
        acc_ref[...] += dot(hidden, wd_buf[slot])

        @pl.when(step + 2 < mlp_steps)
        def _():
            start(mlp_copies(step + 2, slot))

        return carry

    lax.fori_loop(0, mlp_steps, mlp_step, 0)
    send_ref[...] = acc_ref[:half, :]
    keep_ref[...] = mid_ref[own, :] + acc_ref[half:, :]


def chunk_layer(x, chunk, attn_mine, attn_peer, wo_mine, wo_pieces, gain, w_gate, w_up, w_down):
    rows, depth = attn_mine.shape
    dim, ff = w_gate.shape
    width = 512
    whole = lambda a, b: pl.BlockSpec((a, b), lambda i: (0, 0))
    raw = pl.BlockSpec(memory_space=pltpu.HBM)
    pieces = len(wo_pieces)
    return pl.pallas_call(
        functools.partial(chunk_kernel, pieces), name="chunk_layer", grid=(1,),
        in_specs=[pl.BlockSpec((rows, dim), lambda i: (chunk, 0)), whole(rows, depth), whole(rows, depth), whole(1, dim)] + [raw] * (pieces + 4),
        out_specs=[whole(rows // 2, dim)] * 2,
        scratch_shapes=[pltpu.VMEM((rows, dim), F32), pltpu.VMEM((rows, dim), BF16), pltpu.VMEM((rows, dim), F32),
                        pltpu.VMEM((2, depth, width), BF16), pltpu.VMEM((2, depth, width), BF16),
                        pltpu.VMEM((2, dim, FF_BLOCK), BF16), pltpu.VMEM((2, dim, FF_BLOCK), BF16), pltpu.VMEM((2, FF_BLOCK, dim), BF16),
                        pltpu.SemaphoreType.DMA((2, HEAD_GROUPS + pieces)), pltpu.SemaphoreType.DMA((2, 3))],
        out_shape=[jax.ShapeDtypeStruct((rows // 2, dim), F32)] * 2,
        compiler_params=params(("arbitrary",), 60),
        cost_estimate=pl.CostEstimate(flops=4 * rows * depth * dim + 6 * rows * dim * ff, bytes_accessed=6 * dim * ff, transcendentals=0),
    )(x, attn_mine, attn_peer, gain, wo_mine, *wo_pieces, w_gate, w_up, w_down)


def unwritten(shape, dtype):
    return pl.pallas_call(lambda out_ref: None, name="unwritten", out_shape=jax.ShapeDtypeStruct(shape, dtype),
                          out_specs=pl.BlockSpec(memory_space=pltpu.HBM))()


def finish_kernel(meta_ref, kept_ref, sent_ref, y_in, own_ref, y_ref):
    y_own = (kept_ref[...] + sent_ref[...]).astype(BF16)
    own_ref[...] = y_own
    y_ref[...] = y_own


def finish_rows(meta, chunk, kept, sent, y_out):
    rows, dim = kept.shape
    whole = pl.BlockSpec((rows, dim), lambda i, m: (0, 0))
    return pl.pallas_call(
        finish_kernel, name="finish_rows",
        grid_spec=pltpu.PrefetchScalarGridSpec(
            num_scalar_prefetch=1, grid=(1,), in_specs=[whole, whole, pl.BlockSpec(memory_space=pltpu.HBM)],
            out_specs=[whole, pl.BlockSpec((rows, dim), lambda i, m: (2 * chunk + m[2], 0))]),
        out_shape=[jax.ShapeDtypeStruct((rows, dim), BF16), jax.ShapeDtypeStruct(y_out.shape, BF16)],
        input_output_aliases={3: 1},
        compiler_params=params(("arbitrary",), 32),
        cost_estimate=pl.CostEstimate(flops=rows * dim, bytes_accessed=12 * rows * dim, transcendentals=0),
    )(meta, kept, sent, y_out)


def place_kernel(meta_ref, piece_ref, y_in, y_ref):
    y_ref[...] = piece_ref[...]


def place_rows(meta, chunk, piece, y_out):
    rows, dim = piece.shape
    return pl.pallas_call(
        place_kernel, name="place_rows",
        grid_spec=pltpu.PrefetchScalarGridSpec(
            num_scalar_prefetch=1, grid=(1,),
            in_specs=[pl.BlockSpec((rows, dim), lambda i, m: (0, 0)), pl.BlockSpec(memory_space=pltpu.HBM)],
            out_specs=pl.BlockSpec((rows, dim), lambda i, m: (2 * chunk + m[3], 0))),
        out_shape=jax.ShapeDtypeStruct(y_out.shape, BF16),
        input_output_aliases={2: 0},
        compiler_params=params(("arbitrary",), 32),
        cost_estimate=pl.CostEstimate(flops=rows * dim, bytes_accessed=4 * rows * dim, transcendentals=0),
    )(meta, piece, y_out)


def solution(mesh):
    sp_size = mesh.shape["sp"]
    row_spec = P(("rep", "sp"), None)
    tok_spec = P(("rep", "sp"))
    full_spec = P(None)
    col_spec = P(None, "tp")
    wrow_spec = P("tp", None)
    cache_spec = P("rep", ("tp", "sp"), None)
    tp_swap = [(0, 1), (1, 0)]
    core_swap = [(i, i ^ 1) for i in range(sp_size)]
    chip_swap = [(i, i ^ 2) for i in range(sp_size)]

    def layer(x_in, positions, segments, gain_attn, w_q, w_k, w_v, w_o, gain_mlp, w_gate, w_up, w_down):
        rows_local, dim = x_in.shape
        tp_idx, sp_idx = lax.axis_index("tp"), lax.axis_index("sp")
        odd, high = (sp_idx & 1) == 1, (sp_idx & 2) == 2

        depth = w_o.shape[0]
        quarter = depth // sp_size
        half_q = quarter // 2

        def wo_rows(index, second, weights=w_o):
            return lax.dynamic_slice(weights, (index * quarter + second * half_q, 0), (half_q, dim))

        wo_a = lax.ppermute(wo_rows(sp_idx, 0), "tp", tp_swap)

        zeros = jnp.sum((segments == 0).astype(jnp.int32)).reshape(1)
        zeros = zeros + lax.ppermute(zeros, "sp", core_swap)
        cut = (zeros + lax.ppermute(zeros, "sp", chip_swap))[0]
        meta = jnp.stack([sp_idx, cut, tp_idx, 1 - tp_idx]).astype(jnp.int32)

        cos_t, sin_t = rope_tables(positions)
        gain_a, gain_m = gain_attn.reshape(1, dim), gain_mlp.reshape(1, dim)
        u, kv_own = project_kv(x_in, gain_a, w_k, w_v, cos_t, sin_t)
        kv_chip = lax.ppermute(kv_own, "sp", chip_swap)
        kv_core = lax.ppermute(kv_own, "sp", core_swap)
        kv_diag = lax.ppermute(kv_chip, "sp", core_swap)
        kv_parts = (kv_own, kv_core, kv_chip, kv_diag)

        late_w_o, u = lax.optimization_barrier((w_o, u))
        wo_b = lax.ppermute(wo_rows(sp_idx, 1, late_w_o), "tp", tp_swap)
        wo_far = lax.ppermute(wo_rows(sp_idx ^ 2, 1, late_w_o), "tp", tp_swap)
        q_rot = project_q(u, w_q, cos_t, sin_t)
        wo_near = lax.ppermute(wo_a, "sp", chip_swap)
        wo_core = [lax.ppermute(piece, "sp", core_swap) for piece in
                   (wo_a, wo_b, wo_near, wo_far)]
        wo_pieces = (wo_a, wo_b, wo_core[0], wo_core[1], wo_near, wo_far, wo_core[2], wo_core[3])

        def ordered(own, core, chip, diag):
            near = jnp.concatenate([jnp.where(odd, core, own), jnp.where(odd, own, core)], axis=0)
            far = jnp.concatenate([jnp.where(odd, diag, chip), jnp.where(odd, chip, diag)], axis=0)
            return jnp.concatenate([jnp.where(high, far, near), jnp.where(high, near, far)], axis=0)

        def cache(offset):
            cols = [lax.dynamic_slice(part, (0, offset + sp_idx * HEAD_DIM), (rows_local, HEAD_DIM)) for part in kv_parts]
            return ordered(*cols).reshape(sp_size * rows_local, 1, HEAD_DIM)

        chunk_rows = rows_local // CHUNKS
        attn_flops = 4 * chunk_rows * sp_size * rows_local * w_q.shape[1] // 4
        split = CHUNKS // 2
        partial_sums = attention(meta, q_rot, kv_parts[:2], 0, split * chunk_rows, 512, attn_flops, False)
        attn_mine, attn_peer = [], []
        for c in range(CHUNKS):
            if c < split:
                rest = (kv_parts[2:], c * chunk_rows, chunk_rows, 1024, attn_flops, True, partial_sums)
            else:
                rest = (kv_parts, c * chunk_rows, chunk_rows, 1024, attn_flops)
            attn_mine.append(attention(meta, q_rot, *rest))
            attn_peer.append(lax.ppermute(attn_mine[c], "tp", tp_swap))
        k_cache, v_cache = cache(0), cache(w_k.shape[1])
        y_out = unwritten((rows_local, dim), BF16)

        kept, sent = [], []
        for c in range(CHUNKS):
            p_peer, p_own = chunk_layer(x_in, c, attn_mine[c], attn_peer[c], w_o, wo_pieces, gain_m,
                                   w_gate, w_up, w_down)
            sent.append(lax.ppermute(p_peer, "tp", tp_swap))
            kept.append(p_own)
        y_peer = []
        for c in range(CHUNKS):
            y_own, y_out = finish_rows(meta, c, kept[c], sent[c], y_out)
            y_peer.append(lax.ppermute(y_own, "tp", tp_swap))
        for c in range(CHUNKS):
            y_out = place_rows(meta, c, y_peer[c], y_out)
        return y_out, k_cache, v_cache


    return jax.shard_map(layer, mesh=mesh,
                         in_specs=(row_spec, tok_spec, tok_spec, full_spec, col_spec, col_spec, col_spec, wrow_spec,
                                   full_spec, col_spec, col_spec, wrow_spec),
                         out_specs=(row_spec, cache_spec, cache_spec), check_vma=False)
```

```python
import functools
import jax
import jax.numpy as jnp
from jax import lax
from jax.experimental import pallas as pl
from jax.experimental.pallas import tpu as pltpu
from jax.sharding import PartitionSpec as P


HEAD_DIM = 128
HALF = HEAD_DIM // 2
ROPE_BASE = 500000.0
NORM_EPS = 1e-5
LOG2E = 1.4426950408889634
BF16 = jnp.bfloat16
F32 = jnp.float32

CHUNKS = 4
FF_BLOCK = 512
FINE_BLOCK = 512
HEAD_GROUPS = 4
MASKED = -1e30


def params(semantics, mib):
    return pltpu.CompilerParams(dimension_semantics=semantics, vmem_limit_bytes=mib << 20)


def dot(a, b):
    return jnp.dot(a, b, preferred_element_type=F32)


def normed(x, gain):
    mean_sq = jnp.mean(x * x, axis=-1, keepdims=True)
    return (x * lax.rsqrt(mean_sq + NORM_EPS) * gain).astype(BF16)


def rope_tables(positions):
    inv_freq = jnp.power(jnp.float32(ROPE_BASE), -jnp.arange(HALF, dtype=F32) * (2.0 / HEAD_DIM))
    angles = positions.astype(F32)[:, None] * jnp.concatenate([inv_freq, inv_freq])
    sign = jnp.where(jnp.arange(HEAD_DIM) < HALF, -1.0, 1.0).astype(F32)
    return jnp.cos(angles), jnp.sin(angles) * sign


def store_rotated(out_ref, rows, t_f32, cos_t, sin_t):
    for head in range(t_f32.shape[1] // HEAD_DIM):
        cols = slice(head * HEAD_DIM, (head + 1) * HEAD_DIM)
        t_head = t_f32[:, cols]
        out_ref[rows, cols] = (t_head * cos_t + pltpu.roll(t_head, HALF, 1) * sin_t).astype(BF16)


def kv_kernel(x_ref, gain_ref, wk_ref, wv_ref, cos_ref, sin_ref, u_ref, kv_ref):
    u = normed(x_ref[...].astype(F32), gain_ref[...])
    u_ref[...] = u
    width = wk_ref.shape[1]
    store_rotated(kv_ref, slice(None), dot(u, wk_ref[...]), cos_ref[...], sin_ref[...])
    kv_ref[:, width:] = dot(u, wv_ref[...]).astype(BF16)


def project_kv(x, gain, w_k, w_v, cos_t, sin_t):
    rows, dim = x.shape
    width = w_k.shape[1]
    block = 256
    whole = lambda a, b: pl.BlockSpec((a, b), lambda i: (0, 0))
    banded = lambda b: pl.BlockSpec((block, b), lambda i: (i, 0))
    return pl.pallas_call(
        kv_kernel, grid=(rows // block,), name="project_kv",
        in_specs=[banded(dim), whole(1, dim), whole(dim, width), whole(dim, width), banded(HEAD_DIM), banded(HEAD_DIM)],
        out_specs=[banded(dim), banded(2 * width)],
        out_shape=[jax.ShapeDtypeStruct((rows, dim), BF16), jax.ShapeDtypeStruct((rows, 2 * width), BF16)],
        compiler_params=params(("arbitrary",), 48),
        cost_estimate=pl.CostEstimate(flops=4 * rows * dim * width, bytes_accessed=4 * dim * (rows + width), transcendentals=0),
    )(x, gain, w_k, w_v, cos_t, sin_t)


def q_kernel(u_ref, w_ref, cos_ref, sin_ref, q_ref):
    block = 512

    @pl.loop(0, u_ref.shape[0] // block)
    def _(i):
        rows = pl.ds(pl.multiple_of(i * block, block), block)
        store_rotated(q_ref, rows, dot(u_ref[rows, :], w_ref[...]), cos_ref[rows, :], sin_ref[rows, :])


def project_q(u, w_q, cos_t, sin_t, first, rows):
    dim, width = w_q.shape
    block = 512
    banded = lambda b: pl.BlockSpec((rows, b), lambda i: (first // rows, 0))
    return pl.pallas_call(
        q_kernel, grid=(width // block,), name="project_q",
        in_specs=[banded(dim), pl.BlockSpec((dim, block), lambda i: (0, i)), banded(HEAD_DIM), banded(HEAD_DIM)],
        out_specs=pl.BlockSpec((rows, block), lambda i: (0, i)),
        out_shape=jax.ShapeDtypeStruct((rows, width), BF16),
        compiler_params=params(("arbitrary",), 48),
        cost_estimate=pl.CostEstimate(flops=2 * rows * dim * width, bytes_accessed=2 * dim * (rows + width), transcendentals=0),
    )(u, w_q, cos_t, sin_t)


def attn_kernel(group, row_base, parts, k_block, load, finish, meta_ref, q_ref, *refs):
    k_refs, v_refs, refs = refs[:parts], refs[parts:2 * parts], refs[2 * parts:]
    if load:
        acc_in, m_in, l_in = refs[:3]
    if finish:
        o_ref = refs[-7]
    else:
        acc_out, m_out, l_out = refs[:3]
    k_all, v_all, q_t, m_ref, l_ref, acc_ref = refs[-6:]
    shard, cut = meta_ref[0], meta_ref[1]
    block = q_ref.shape[0]
    keys = k_refs[0].shape[0]
    scale = (HEAD_DIM ** -0.5) * LOG2E
    chip_base = (shard // 2) * (2 * keys)
    base = 0 if finish else chip_base

    @pl.when(pl.program_id(1) == 0)
    def _():
        for idx in range(parts):
            rows = pl.ds(pl.multiple_of(((shard ^ idx) & (parts - 1)) * keys, keys), keys)
            k_all[rows, :] = k_refs[idx][...]
            v_all[:, rows] = v_refs[idx][...].T

    first = shard * keys + row_base + pl.program_id(1) * block
    last = first + block - 1
    for head in range(group):
        q_t[head] = q_ref[:, head * HEAD_DIM:(head + 1) * HEAD_DIM].T
    if load:
        m_ref[...], l_ref[...], acc_ref[...] = m_in[...], l_in[...], acc_in[...]
    else:
        m_ref[...] = jnp.full_like(m_ref, MASKED)
        l_ref[...] = jnp.zeros_like(l_ref)
        acc_ref[...] = jnp.zeros_like(acc_ref)

    fine = min(k_block, FINE_BLOCK)

    def step(masked, kb, carry):
        size = fine if masked else k_block
        start = kb * size
        rows = pl.ds(pl.multiple_of(start - base, size), size)
        k_blk = k_all[rows, :]
        v_blk = v_all[:, rows]
        scores = [dot(k_blk, q_t[head]) for head in range(group)]
        m_old = [m_ref[head] for head in range(group)]
        l_old = [l_ref[head] for head in range(group)]
        if masked:
            k_idx = start + lax.broadcasted_iota(jnp.int32, (size, block), 0)
            r_idx = first + lax.broadcasted_iota(jnp.int32, (size, block), 1)
            allowed = (k_idx <= r_idx) & ((k_idx >= cut) | (r_idx < cut))
            scores = [jnp.where(allowed, s, MASKED) for s in scores]
        news = []
        for head in range(group):
            m_new = jnp.maximum(m_old[head], jnp.max(scores[head], axis=0, keepdims=True) * scale)
            p = jnp.exp2(scores[head] * scale - m_new)
            alpha = jnp.exp2(m_old[head] - m_new)
            total = alpha * l_old[head] + jnp.sum(p, axis=0, keepdims=True)
            news.append((m_new, total, alpha, dot(v_blk, p.astype(BF16))))
        for head in range(group):
            m_ref[head], l_ref[head] = news[head][:2]
            acc_ref[head] = news[head][2] * acc_ref[head] + news[head][3]
        return carry

    seg_low = jnp.where(first >= cut, cut, 0)
    seg_high = jnp.where(last >= cut, cut, 0)
    low = jnp.maximum(seg_low, base) // k_block
    high = chip_base // k_block if load else last // k_block + 1
    clear = (seg_high + k_block - 1) // k_block
    edge_a = jnp.maximum(low, jnp.minimum(clear, high))
    edge_b = jnp.maximum(edge_a, jnp.minimum((first + 1) // k_block, high))
    lax.fori_loop(edge_a, edge_b, functools.partial(step, False), 0)
    ratio = k_block // fine
    fine_low = jnp.maximum(seg_low, base) // fine
    fine_high = chip_base // fine if load else last // fine + 1
    head_count = jnp.maximum(jnp.minimum(edge_a * ratio, fine_high) - fine_low, 0)
    fine_rest = jnp.maximum(edge_b * ratio, fine_low)
    lax.fori_loop(0, head_count + jnp.maximum(fine_high - fine_rest, 0),
                  lambda i, carry: step(True, jnp.where(i < head_count, fine_low + i, fine_rest + i - head_count), carry), 0)
    if finish:
        for head in range(group):
            o_ref[:, head * HEAD_DIM:(head + 1) * HEAD_DIM] = (acc_ref[head] / l_ref[head]).T.astype(BF16)
    else:
        acc_out[...], m_out[...], l_out[...] = acc_ref[...], m_ref[...], l_ref[...]


def attention(meta, q_rot, q_base, kv_parts, row_base, rows, q_block, k_block, flops, finish=True, partial_sums=None):
    kv_rows, kv_width = kv_parts[0].shape
    kv_heads = kv_width // (2 * HEAD_DIM)
    group = q_rot.shape[1] // HEAD_DIM // kv_heads
    width = group * HEAD_DIM
    base = row_base // q_block
    parts, load = len(kv_parts), partial_sums is not None
    k_spec = pl.BlockSpec((kv_rows, HEAD_DIM), lambda h, i, m: (0, h))
    v_spec = pl.BlockSpec((kv_rows, HEAD_DIM), lambda h, i, m: (0, kv_heads + h))
    sums_specs = [pl.BlockSpec((group, depth, q_block), lambda h, i, m: (h, 0, base + i)) for depth in (HEAD_DIM, 1, 1)]
    sums_shapes = [jax.ShapeDtypeStruct((kv_heads * group, depth, rows), F32) for depth in (HEAD_DIM, 1, 1)]
    return pl.pallas_call(
        functools.partial(attn_kernel, group, row_base, parts, k_block, load, finish), name="attention",
        grid_spec=pltpu.PrefetchScalarGridSpec(
            num_scalar_prefetch=1, grid=(kv_heads, rows // q_block),
            in_specs=[pl.BlockSpec((q_block, width), lambda h, i, m: (q_base // q_block + i, h))] + [k_spec] * parts + [v_spec] * parts
                     + (sums_specs if load else []),
            out_specs=pl.BlockSpec((q_block, width), lambda h, i, m: (i, h ^ m[0])) if finish else sums_specs,
            scratch_shapes=[pltpu.VMEM((parts * kv_rows, HEAD_DIM), BF16), pltpu.VMEM((HEAD_DIM, parts * kv_rows), BF16),
                            pltpu.VMEM((group, HEAD_DIM, q_block), BF16), pltpu.VMEM((group, 1, q_block), F32),
                            pltpu.VMEM((group, 1, q_block), F32), pltpu.VMEM((group, HEAD_DIM, q_block), F32)]),
        out_shape=jax.ShapeDtypeStruct((rows, kv_heads * width), BF16) if finish else sums_shapes,
        compiler_params=params(("arbitrary", "arbitrary"), 48),
        cost_estimate=pl.CostEstimate(flops=flops, bytes_accessed=16 << 20, transcendentals=0),
    )(meta, q_rot, *kv_parts, *kv_parts, *(partial_sums or ()))


def chunk_kernel(pieces, x_ref, a_ref, b_ref, gain_ref, wo_ref, *refs):
    piece_refs, (wg_ref, wu_ref, wd_ref, send_ref, keep_ref) = refs[:pieces], refs[pieces:pieces + 5]
    mid_ref, u_ref, wa_buf, wb_buf, wg_buf, wu_buf, wd_buf, wo_sem, mlp_sem = refs[pieces + 5:]
    tp_idx, sp_idx = lax.axis_index("tp"), lax.axis_index("sp")
    half = send_ref.shape[0]
    depth, width = wa_buf.shape[1:]
    quarter = depth // HEAD_GROUPS
    out_steps = wo_ref.shape[1] // width
    mlp_steps = wg_ref.shape[1] // FF_BLOCK

    def wo_copies(step, slot):
        cols = pl.ds(pl.multiple_of(step * width, width), width)
        copies, top = [], 0
        for p in range(HEAD_GROUPS):
            rows = pl.ds(pl.multiple_of((p ^ sp_idx) * quarter, quarter), quarter)
            copies.append((wo_ref.at[rows, cols], wa_buf.at[slot, p * quarter:(p + 1) * quarter, :]))
        for piece in piece_refs:
            rows = piece.shape[0]
            copies.append((piece.at[:, cols], wb_buf.at[slot, top:top + rows, :]))
            top += rows
        return [pltpu.make_async_copy(src, dst, wo_sem.at[slot, n]) for n, (src, dst) in enumerate(copies)]

    def mlp_copies(step, slot):
        cols = pl.ds(pl.multiple_of(step * FF_BLOCK, FF_BLOCK), FF_BLOCK)
        copies = ((wg_ref.at[:, cols], wg_buf.at[slot]), (wu_ref.at[:, cols], wu_buf.at[slot]), (wd_ref.at[cols, :], wd_buf.at[slot]))
        return [pltpu.make_async_copy(src, dst, mlp_sem.at[slot, n]) for n, (src, dst) in enumerate(copies)]

    def start(copies):
        for copy in copies:
            copy.start()

    def finish(copies):
        for copy in copies:
            copy.wait()

    start(wo_copies(0, 0))
    start(wo_copies(1, 1))
    send_ref[...] = jnp.zeros_like(send_ref)

    def out_step(step, carry):
        slot = step % 2
        finish(wo_copies(step, slot))
        cols = pl.ds(pl.multiple_of(step * width, width), width)
        mid_ref[:, cols] = x_ref[:, cols].astype(F32) + (dot(a_ref[...], wa_buf[slot]) + dot(b_ref[...], wb_buf[slot]))

        @pl.when(step + 2 < out_steps)
        def _():
            start(wo_copies(step + 2, slot))

        @pl.when(step == out_steps - 3)
        def _():
            start(mlp_copies(0, 0))

        return carry

    lax.fori_loop(0, out_steps, out_step, 0)
    start(mlp_copies(1, 1))

    keep_ref[...] = mid_ref[pl.ds(pl.multiple_of(tp_idx * half, half), half), :]

    @pl.loop(0, 2)
    def _(i):
        u_ref[pl.ds(pl.multiple_of(i * half, half), half), :] = normed(
            mid_ref[pl.ds(pl.multiple_of((tp_idx ^ i ^ 1) * half, half), half), :], gain_ref[...])

    def mlp_step(step, carry):
        slot = step % 2
        finish(mlp_copies(step, slot))
        u = u_ref[...]
        gate = dot(u, wg_buf[slot])
        hidden = (gate * jax.nn.sigmoid(gate) * dot(u, wu_buf[slot])).astype(BF16)
        added = dot(hidden, wd_buf[slot])
        send_ref[...] += added[:half, :]
        keep_ref[...] += added[half:, :]

        @pl.when(step + 2 < mlp_steps)
        def _():
            start(mlp_copies(step + 2, slot))

        return carry

    lax.fori_loop(0, mlp_steps, mlp_step, 0)


def chunk_layer(x, chunk, attn_mine, attn_peer, wo_mine, wo_pieces, gain, w_gate, w_up, w_down):
    rows, depth = attn_mine.shape
    dim, ff = w_gate.shape
    width = 512
    whole = lambda a, b: pl.BlockSpec((a, b), lambda i: (0, 0))
    raw = pl.BlockSpec(memory_space=pltpu.HBM)
    pieces = len(wo_pieces)
    return pl.pallas_call(
        functools.partial(chunk_kernel, pieces), name="chunk_layer", grid=(1,),
        in_specs=[pl.BlockSpec((rows, dim), lambda i: (chunk, 0)), whole(rows, depth), whole(rows, depth), whole(1, dim)] + [raw] * (pieces + 4),
        out_specs=[whole(rows // 2, dim)] * 2,
        scratch_shapes=[pltpu.VMEM((rows, dim), F32), pltpu.VMEM((rows, dim), BF16),
                        pltpu.VMEM((2, depth, width), BF16), pltpu.VMEM((2, depth, width), BF16),
                        pltpu.VMEM((2, dim, FF_BLOCK), BF16), pltpu.VMEM((2, dim, FF_BLOCK), BF16), pltpu.VMEM((2, FF_BLOCK, dim), BF16),
                        pltpu.SemaphoreType.DMA((2, HEAD_GROUPS + pieces)), pltpu.SemaphoreType.DMA((2, 3))],
        out_shape=[jax.ShapeDtypeStruct((rows // 2, dim), F32)] * 2,
        compiler_params=params(("arbitrary",), 60),
        cost_estimate=pl.CostEstimate(flops=4 * rows * depth * dim + 6 * rows * dim * ff, bytes_accessed=6 * dim * ff, transcendentals=0),
    )(x, attn_mine, attn_peer, gain, wo_mine, *wo_pieces, w_gate, w_up, w_down)


def unwritten(shape, dtype):
    return pl.pallas_call(lambda out_ref: None, name="unwritten", out_shape=jax.ShapeDtypeStruct(shape, dtype),
                          out_specs=pl.BlockSpec(memory_space=pltpu.HBM))()


def finish_kernel(meta_ref, kept_ref, sent_ref, y_in, own_ref, y_ref):
    y_own = (kept_ref[...] + sent_ref[...]).astype(BF16)
    own_ref[...] = y_own
    y_ref[...] = y_own


def finish_rows(meta, chunk, kept, sent, y_out):
    rows, dim = kept.shape
    whole = pl.BlockSpec((rows, dim), lambda i, m: (0, 0))
    return pl.pallas_call(
        finish_kernel, name="finish_rows",
        grid_spec=pltpu.PrefetchScalarGridSpec(
            num_scalar_prefetch=1, grid=(1,), in_specs=[whole, whole, pl.BlockSpec(memory_space=pltpu.HBM)],
            out_specs=[whole, pl.BlockSpec((rows, dim), lambda i, m: (2 * chunk + m[2], 0))]),
        out_shape=[jax.ShapeDtypeStruct((rows, dim), BF16), jax.ShapeDtypeStruct(y_out.shape, BF16)],
        input_output_aliases={3: 1},
        compiler_params=params(("arbitrary",), 32),
        cost_estimate=pl.CostEstimate(flops=rows * dim, bytes_accessed=12 * rows * dim, transcendentals=0),
    )(meta, kept, sent, y_out)


def place_kernel(meta_ref, piece_ref, y_in, y_ref):
    y_ref[...] = piece_ref[...]


def place_rows(meta, chunk, piece, y_out):
    rows, dim = piece.shape
    return pl.pallas_call(
        place_kernel, name="place_rows",
        grid_spec=pltpu.PrefetchScalarGridSpec(
            num_scalar_prefetch=1, grid=(1,),
            in_specs=[pl.BlockSpec((rows, dim), lambda i, m: (0, 0)), pl.BlockSpec(memory_space=pltpu.HBM)],
            out_specs=pl.BlockSpec((rows, dim), lambda i, m: (2 * chunk + m[3], 0))),
        out_shape=jax.ShapeDtypeStruct(y_out.shape, BF16),
        input_output_aliases={2: 0},
        compiler_params=params(("arbitrary",), 32),
        cost_estimate=pl.CostEstimate(flops=rows * dim, bytes_accessed=4 * rows * dim, transcendentals=0),
    )(meta, piece, y_out)


def solution(mesh):
    sp_size = mesh.shape["sp"]
    row_spec = P(("rep", "sp"), None)
    tok_spec = P(("rep", "sp"))
    full_spec = P(None)
    col_spec = P(None, "tp")
    wrow_spec = P("tp", None)
    cache_spec = P("rep", ("tp", "sp"), None)
    tp_swap = [(0, 1), (1, 0)]
    core_swap = [(i, i ^ 1) for i in range(sp_size)]
    chip_swap = [(i, i ^ 2) for i in range(sp_size)]

    def layer(x_in, positions, segments, gain_attn, w_q, w_k, w_v, w_o, gain_mlp, w_gate, w_up, w_down):
        rows_local, dim = x_in.shape
        tp_idx, sp_idx = lax.axis_index("tp"), lax.axis_index("sp")
        odd, high = (sp_idx & 1) == 1, (sp_idx & 2) == 2

        depth = w_o.shape[0]
        quarter = depth // sp_size
        half_q = quarter // 2

        def wo_rows(index, second, weights=w_o):
            return lax.dynamic_slice(weights, (index * quarter + second * half_q, 0), (half_q, dim))

        wo_a = lax.ppermute(wo_rows(sp_idx, 0), "tp", tp_swap)

        zeros = jnp.sum((segments == 0).astype(jnp.int32)).reshape(1)
        zeros = zeros + lax.ppermute(zeros, "sp", core_swap)
        cut = (zeros + lax.ppermute(zeros, "sp", chip_swap))[0]
        meta = jnp.stack([sp_idx, cut, tp_idx, 1 - tp_idx]).astype(jnp.int32)

        cos_t, sin_t = rope_tables(positions)
        gain_a, gain_m = gain_attn.reshape(1, dim), gain_mlp.reshape(1, dim)
        u, kv_own = project_kv(x_in, gain_a, w_k, w_v, cos_t, sin_t)
        kv_chip = lax.ppermute(kv_own, "sp", chip_swap)
        kv_core = lax.ppermute(kv_own, "sp", core_swap)
        kv_diag = lax.ppermute(kv_chip, "sp", core_swap)
        kv_parts = (kv_own, kv_core, kv_chip, kv_diag)

        late_w_o, u = lax.optimization_barrier((w_o, u))
        wo_b = lax.ppermute(wo_rows(sp_idx, 1, late_w_o), "tp", tp_swap)
        wo_far = lax.ppermute(wo_rows(sp_idx ^ 2, 1, late_w_o), "tp", tp_swap)
        chunk_rows = rows_local // CHUNKS
        q_rot = project_q(u, w_q, cos_t, sin_t, 0, rows_local)
        wo_near = lax.ppermute(wo_a, "sp", chip_swap)
        wo_core = [lax.ppermute(piece, "sp", core_swap) for piece in
                   (wo_a, wo_b, wo_near, wo_far)]
        wo_pieces = (wo_a, wo_b, wo_core[0], wo_core[1], wo_near, wo_far, wo_core[2], wo_core[3])

        def ordered(own, core, chip, diag):
            near = jnp.concatenate([jnp.where(odd, core, own), jnp.where(odd, own, core)], axis=0)
            far = jnp.concatenate([jnp.where(odd, diag, chip), jnp.where(odd, chip, diag)], axis=0)
            return jnp.concatenate([jnp.where(high, far, near), jnp.where(high, near, far)], axis=0)

        def cache(offset):
            cols = [lax.dynamic_slice(part, (0, offset + sp_idx * HEAD_DIM), (rows_local, HEAD_DIM)) for part in kv_parts]
            return ordered(*cols).reshape(sp_size * rows_local, 1, HEAD_DIM)

        attn_flops = 4 * chunk_rows * sp_size * rows_local * w_q.shape[1] // 4
        split = CHUNKS // 2
        partial_sums = attention(meta, q_rot, 0, kv_parts[:2], 0, split * chunk_rows, split * chunk_rows, 512, attn_flops, False)
        attn_mine, attn_peer = [], []
        for c in range(CHUNKS):
            if c < split:
                rest = (kv_parts[2:], c * chunk_rows, chunk_rows, chunk_rows, 1024, attn_flops, True, partial_sums)
            else:
                rest = (kv_parts, c * chunk_rows, chunk_rows, chunk_rows, 1024, attn_flops)
            attn_mine.append(attention(meta, q_rot, c * chunk_rows, *rest))
            attn_peer.append(lax.ppermute(attn_mine[c], "tp", tp_swap))
        k_cache, v_cache = cache(0), cache(w_k.shape[1])
        y_out = unwritten((rows_local, dim), BF16)

        kept, sent = [], []
        for c in range(CHUNKS):
            p_peer, p_own = chunk_layer(x_in, c, attn_mine[c], attn_peer[c], w_o, wo_pieces, gain_m,
                                   w_gate, w_up, w_down)
            sent.append(lax.ppermute(p_peer, "tp", tp_swap))
            kept.append(p_own)
        y_peer = []
        for c in range(CHUNKS):
            y_own, y_out = finish_rows(meta, c, kept[c], sent[c], y_out)
            y_peer.append(lax.ppermute(y_own, "tp", tp_swap))
        for c in range(CHUNKS):
            y_out = place_rows(meta, c, y_peer[c], y_out)
        return y_out, k_cache, v_cache


    return jax.shard_map(layer, mesh=mesh,
                         in_specs=(row_spec, tok_spec, tok_spec, full_spec, col_spec, col_spec, col_spec, wrow_spec,
                                   full_spec, col_spec, col_spec, wrow_spec),
                         out_specs=(row_spec, cache_spec, cache_spec), check_vma=False)
```
